32 devices in a mesh: ta: 16 (over z, y, core), ka: 2 (over x).
Axes of the slice: x: 2, y: 2, z: 4, core: 2. Of those that a mesh axis runs over, the one named last changes fastest.
Arguments:
- green_row: float32 [2, 4, 4, 32, 1024], P(None, None, None, 'ta', 'ka'), may hold values from -6 to 6
- screen_lesser: float32 [2, 4, 4, 32, 1024], P(None, None, None, 'ta', 'ka'), may hold values from -6 to 6
- screen_retarded: float32 [2, 4, 4, 32, 1024], P(None, None, None, 'ta', 'ka'), may hold values from -6 to 6
- onsite: float32 [2, 4, 4], replicated, may hold values from -3 to 3
- lesser_slab: bfloat16 [2, 4, 4, 32, 32, 1024], P(None, None, None, 'ta', None, 'ka'), may hold values from -0.5 to 0.5
- advanced_slab: bfloat16 [2, 4, 4, 32, 32, 1024], P(None, None, None, 'ta', None, 'ka'), may hold values from -0.5 to 0.5
- slab_start: int32 [1], replicated, may hold values from 0 to 4095
- block_table: int32 [16], replicated, may hold values from 0 to 15, each once
Outputs:
- next_row: float32 [2, 4, 4, 32, 1024], P(None, None, None, 'ta', 'ka')
- derivative: float32 [2, 4, 4, 32, 1024], P(None, None, None, 'ta', 'ka')
The draws below stay inside these ranges and needn't reach their ends.
Inputs may be any that keep to these rules, and one draw needn't show every extreme that they name: block_table is a permutation: each time block 0 to 15 appears once.
All inputs are finite; a program needn't handle non-finite values.
Results may differ from the reference program's by a relative error of at most 0.0019.
Values sent between devices are 32-bit elements; how exact they have to be, the bound alone decides.
No kernel may reach another device: no remote copies, remote signals or barrier semaphores. Data moves between devices by JAX's collectives and lax.ppermute only.
A program may use at most 128 MiB of HBM per device.

```python
import math
import jax
import jax.numpy as jnp
from jax import lax

ORB = 4
KS = 32
T_DEV = 2
K = 1024
TIMES = 32
N_TA = 16


def strengthened(values, key, source, target, shards_of, factor):
    owner, partner = [(jnp.arange(values.shape[dim]) // (values.shape[dim] // shards_of)).reshape([-1 if axis == dim else 1 for axis in range(values.ndim)]) for dim in (source, target)]
    chosen = jax.random.permutation(key, shards_of)[partner]
    strong = (owner == chosen) | (owner == (partner + shards_of // 2) % shards_of)
    return jnp.where(strong, factor * values, values)


def block_scale(rng, extent, shards, low, top_value):
    level, own = 1.0, jax.random.fold_in(rng, 6)
    for position, shards_of in shards:
        heights = jnp.exp(jax.random.uniform(jax.random.fold_in(own, position), (shards_of,), jnp.float32, low / len(shards), top_value / len(shards)))
        level = level * jnp.repeat(heights, extent[position] // shards_of).reshape([-1 if axis == position else 1 for axis in range(len(extent))])
    return level


def gaussian(own_key, dims, deviation, limit, pieces=(), kind=jnp.bfloat16):
    entries = jax.random.normal(own_key, dims, jnp.float32) * deviation
    if len(pieces) > 0:
        entries = block_scale(own_key, dims, pieces, -0.22, 0.18) * entries
    return jnp.clip(entries, min=-limit, max=limit).astype(kind)


def bell_draw_with(key, extent, spread, most, pieces, heavy, held_as=jnp.bfloat16):
    entries = spread * jax.random.normal(key, extent, jnp.float32)
    if pieces:
        entries = entries * block_scale(key, extent, pieces, -0.22, 0.18)
    return jnp.clip(strengthened(entries, jax.random.fold_in(key, 3), *heavy), -most, most).astype(held_as)


def setup_inputs(seed: int = 0) -> dict:
    keys = jax.random.split(jax.random.key(seed), 9)
    return {
        "green_row": gaussian(keys[0], (2, ORB, ORB, TIMES, K), 1.0, 6.0, ((3, 16), (4, 2)), jnp.float32),
        "screen_lesser": gaussian(keys[1], (2, ORB, ORB, TIMES, K), 1.0, 6.0, ((3, 16), (4, 2)), jnp.float32),
        "screen_retarded": gaussian(keys[2], (2, ORB, ORB, TIMES, K), 1.0, 6.0, ((3, 16), (4, 2)), jnp.float32),
        "onsite": gaussian(keys[3], (2, ORB, ORB), 0.5, 3.0, (), jnp.float32),
        "lesser_slab": bell_draw_with(keys[4], (2, ORB, ORB, TIMES, TIMES, K), (2 * ORB * TIMES) ** -0.5, 0.5, ((3, 16), (5, 2)), (3, 4, 16, 2.0)),
        "advanced_slab": bell_draw_with(keys[5], (2, ORB, ORB, TIMES, TIMES, K), (2 * ORB * TIMES) ** -0.5, 0.5, ((3, 16), (5, 2)), (3, 4, 16, 2.0)),
        "slab_start": jax.random.randint(keys[6], (1,), 0, 4096).astype(jnp.int32),
        "block_table": jax.random.permutation(keys[7], N_TA).astype(jnp.int32),
    }


time_step = 0.1
drive_amp = 1.0
drive_freq = 0.37
highest = lax.Precision.HIGHEST

def phase_table(row_ids, col_ids, sign_value):
    products = row_ids[:, None] * col_ids[None, :] % KS
    angle = products.astype(jnp.float32) * (2.0 * math.pi / KS)
    factor = 1.0 / math.sqrt(KS)
    return (jnp.cos(angle) * factor, sign_value * jnp.sin(angle) * factor)

def along_last(values_in, cosine, sine_part):
    real_part = jnp.einsum('...m,mn->...n', values_in[0], cosine, precision=highest) - jnp.einsum('...m,mn->...n', values_in[1], sine_part, precision=highest)
    imag_part = jnp.einsum('...m,mn->...n', values_in[0], sine_part, precision=highest) + jnp.einsum('...m,mn->...n', values_in[1], cosine, precision=highest)
    return jnp.stack([real_part, imag_part])

def along_second(values_in, cosine, sine_part):
    real_part = jnp.einsum('...mj,mn->...nj', values_in[0], cosine, precision=highest) - jnp.einsum('...mj,mn->...nj', values_in[1], sine_part, precision=highest)
    imag_part = jnp.einsum('...mj,mn->...nj', values_in[0], sine_part, precision=highest) + jnp.einsum('...mj,mn->...nj', values_in[1], cosine, precision=highest)
    return jnp.stack([real_part, imag_part])

def transform(values_in, sign_value):
    full_shape = values_in.shape
    grid = values_in.reshape(full_shape[:-1] + (KS, KS))
    numbers = jnp.arange(KS, dtype=jnp.int32)
    cosine, sine_part = phase_table(numbers, numbers, sign_value)
    grid = along_last(grid, cosine, sine_part)
    grid = along_second(grid, cosine, sine_part)
    return grid.reshape(full_shape)

def self_energy(row_space, screens):
    green_real = row_space[0][None]
    green_imag = row_space[1][None]
    real_part = -(green_real * screens[1] + green_imag * screens[0])
    imag_part = green_real * screens[0] - green_imag * screens[1]
    return jnp.stack([real_part, imag_part])

def coupling(sigma_pair):
    return jnp.stack([jnp.stack([sigma_pair[0], -sigma_pair[1]]), jnp.stack([sigma_pair[1], sigma_pair[0]])])

def dispersion(slab_start, kx_ids, ky_ids):
    current = (slab_start[0] + TIMES).astype(jnp.float32)
    shift = drive_amp * jnp.sin(drive_freq * current)
    factor = 2.0 * math.pi / KS
    return -2.0 * (jnp.cos(kx_ids.astype(jnp.float32) * factor + shift) + jnp.cos(ky_ids.astype(jnp.float32) * factor))

def apply_h(row, onsite, energy):
    real_part = jnp.einsum('ab,bctk->actk', onsite[0], row[0], precision=highest) - jnp.einsum('ab,bctk->actk', onsite[1], row[1], precision=highest) + energy * row[0]
    imag_part = jnp.einsum('ab,bctk->actk', onsite[0], row[1], precision=highest) + jnp.einsum('ab,bctk->actk', onsite[1], row[0], precision=highest) + energy * row[1]
    return jnp.stack([real_part, imag_part])

def collide(ret_coupling, less_coupling, lesser_slab, advanced_slab, causal):
    block = math.gcd(K, 128)

    def one_block(counter):
        begin = counter * block
        part_ret = lax.dynamic_slice_in_dim(ret_coupling, begin, block, 5).astype(jnp.float32)
        part_less = lax.dynamic_slice_in_dim(less_coupling, begin, block, 5).astype(jnp.float32)
        slab_one = lax.dynamic_slice_in_dim(lesser_slab, begin, block, 5).astype(jnp.float32)
        slab_two = lax.dynamic_slice_in_dim(advanced_slab, begin, block, 5).astype(jnp.float32) * causal[:, :, None]
        return jnp.einsum('pqabsk,qbcstk->pactk', part_ret, slab_one) + jnp.einsum('pqabsk,qbcstk->pactk', part_less, slab_two)
    blocks = lax.map(one_block, jnp.arange(K // block, dtype=jnp.int32))
    return jnp.moveaxis(blocks, 0, -2).reshape((2, ORB, ORB, TIMES, K))

def reference(green_row, screen_lesser, screen_retarded, onsite, lesser_slab, advanced_slab, slab_start, block_table):
    offsets = jnp.arange(TIMES, dtype=jnp.int32)
    times_abs = jnp.repeat(block_table, T_DEV) * T_DEV + offsets % T_DEV
    causal = (times_abs[:, None] <= times_abs[None, :]).astype(jnp.float32)
    momenta = jnp.arange(K, dtype=jnp.int32)
    energy = dispersion(slab_start, momenta // KS, momenta % KS)
    screens = transform(jnp.stack([screen_lesser, screen_retarded], axis=1), 1.0)

    def rate_of(row):
        row_space = transform(row, 1.0)
        sigma_all = transform(self_energy(row_space, screens), -1.0).astype(jnp.bfloat16)
        collision = collide(coupling(sigma_all[:, 1]), coupling(sigma_all[:, 0]), lesser_slab, advanced_slab, causal)
        totals = apply_h(row, onsite, energy) + collision
        return jnp.stack([totals[1], -totals[0]])
    first_rate = rate_of(green_row)
    estimate = green_row + time_step * first_rate
    latest = first_rate
    for corrector in range(2):
        latest = rate_of(estimate)
        estimate = green_row + 0.5 * time_step * (first_rate + latest)
    return (estimate, latest)
```

```python
import functools
import math

import jax
import jax.numpy as jnp
import numpy as np
from jax import lax
from jax.experimental import pallas as pl
from jax.experimental.pallas import tpu as pltpu
from jax.sharding import PartitionSpec as P

KS = 32
LANES = 128
SUBLANES = 8


time_step = 0.1
drive_amp = 1.0
drive_freq = 0.37
highest = lax.Precision.HIGHEST


def phase_table(row_ids, col_ids, sign_value):
    products = row_ids[:, None] * col_ids[None, :] % KS
    angle = products.astype(jnp.float32) * (2.0 * math.pi / KS)
    factor = 1.0 / math.sqrt(KS)
    return (jnp.cos(angle) * factor, sign_value * jnp.sin(angle) * factor)


def along_last(values_in, cosine, sine_part):
    real_part = jnp.einsum("...m,mn->...n", values_in[0], cosine, precision=highest) - jnp.einsum(
        "...m,mn->...n", values_in[1], sine_part, precision=highest
    )
    imag_part = jnp.einsum(
        "...m,mn->...n", values_in[0], sine_part, precision=highest
    ) + jnp.einsum("...m,mn->...n", values_in[1], cosine, precision=highest)
    return jnp.stack([real_part, imag_part])


def along_second(values_in, cosine, sine_part):
    real_part = jnp.einsum("...mj,mn->...nj", values_in[0], cosine, precision=highest) - jnp.einsum(
        "...mj,mn->...nj", values_in[1], sine_part, precision=highest
    )
    imag_part = jnp.einsum(
        "...mj,mn->...nj", values_in[0], sine_part, precision=highest
    ) + jnp.einsum("...mj,mn->...nj", values_in[1], cosine, precision=highest)
    return jnp.stack([real_part, imag_part])


def transform(values_in, sign_value, ka_index):
    leading = values_in.shape[:-1]
    x_local = values_in.shape[-1] // KS
    numbers = jnp.arange(KS, dtype=jnp.int32)
    owned = ka_index * x_local + jnp.arange(x_local, dtype=jnp.int32)
    cosine, sine_part = phase_table(numbers, numbers, sign_value)
    partly = along_last(values_in.reshape(leading + (x_local, KS)), cosine, sine_part)
    gathered = lax.all_gather(partly.reshape(values_in.shape), "ka", axis=5, tiled=True)
    grid = gathered.reshape(leading + (KS, KS))
    col_cos, col_sin = phase_table(numbers, owned, sign_value)
    return along_second(grid, col_cos, col_sin).reshape(values_in.shape)


def self_energy(row_space, screens):
    green_real = row_space[0][None]
    green_imag = row_space[1][None]
    real_part = -(green_real * screens[1] + green_imag * screens[0])
    imag_part = green_real * screens[0] - green_imag * screens[1]
    return jnp.stack([real_part, imag_part])


def coupling(sigma_pair):
    return jnp.stack(
        [jnp.stack([sigma_pair[0], -sigma_pair[1]]), jnp.stack([sigma_pair[1], sigma_pair[0]])]
    )


def dispersion(slab_start, all_times, kx_ids, ky_ids):
    current = (slab_start[0] + all_times).astype(jnp.float32)
    shift = drive_amp * jnp.sin(drive_freq * current)
    factor = 2.0 * math.pi / KS
    return -2.0 * (
        jnp.cos(kx_ids.astype(jnp.float32) * factor + shift)
        + jnp.cos(ky_ids.astype(jnp.float32) * factor)
    )


def apply_h(row, onsite, energy):
    real_part = (
        jnp.einsum("ab,bctk->actk", onsite[0], row[0], precision=highest)
        - jnp.einsum("ab,bctk->actk", onsite[1], row[1], precision=highest)
        + energy * row[0]
    )
    imag_part = (
        jnp.einsum("ab,bctk->actk", onsite[0], row[1], precision=highest)
        + jnp.einsum("ab,bctk->actk", onsite[1], row[0], precision=highest)
        + energy * row[1]
    )
    return jnp.stack([real_part, imag_part])


def masked_product(less_coupling, row_times, piece_times, piece_adv):
    visible = row_times[:, None] <= piece_times[None, :]
    masked = jnp.where(visible[:, :, None], piece_adv, jnp.zeros_like(piece_adv))
    return jnp.einsum(
        "pqabsk,qbcstk->tpack", less_coupling, masked, preferred_element_type=jnp.float32
    )


def plain(
    green_row,
    screen_lesser,
    screen_retarded,
    onsite,
    lesser_slab,
    advanced_slab,
    slab_start,
    block_table,
):
    local_rows = green_row.shape[3]
    k_local = green_row.shape[4]
    ta_count = lax.axis_size("ta")
    all_times = local_rows * ta_count
    my_index = lax.axis_index("ta")
    ka_index = lax.axis_index("ka")
    my_block = lax.dynamic_slice_in_dim(block_table, my_index, 1)[0]
    row_times = my_block * local_rows + jnp.arange(local_rows, dtype=jnp.int32)
    col_times = jnp.repeat(block_table, local_rows) * local_rows + jnp.tile(
        jnp.arange(local_rows, dtype=jnp.int32), ta_count
    )
    momenta = ka_index * k_local + jnp.arange(k_local, dtype=jnp.int32)
    energy = dispersion(slab_start, all_times, momenta // KS, momenta % KS)
    first_space = transform(
        jnp.stack([screen_lesser, screen_retarded, green_row], axis=1), 1.0, ka_index
    )
    screens = first_space[:, 0:2]

    def rate_of(row, row_space):
        sigma_all = transform(self_energy(row_space, screens), -1.0, ka_index).astype(jnp.bfloat16)
        less_coupling = coupling(sigma_all[:, 0])
        ret_coupling = coupling(sigma_all[:, 1])
        totals = jnp.einsum(
            "pqabsk,qbcstk->tpack", ret_coupling, lesser_slab, preferred_element_type=jnp.float32
        )
        own_rows = lax.psum_scatter(
            totals + masked_product(less_coupling, row_times, col_times, advanced_slab),
            "ta",
            scatter_dimension=0,
            tiled=True,
        )
        collision = jnp.transpose(own_rows, (1, 2, 3, 0, 4))
        totals = apply_h(row, onsite, energy) + collision
        return jnp.stack([totals[1], -totals[0]])

    first_rate = rate_of(green_row, first_space[:, 2])
    estimate = green_row + time_step * first_rate
    latest = first_rate
    for corrector in range(2):
        row_space = transform(estimate[:, None], 1.0, ka_index)[:, 0]
        latest = rate_of(estimate, row_space)
        estimate = green_row + 0.5 * time_step * (first_rate + latest)
    return (estimate, latest)


def halving(size):
    return size > 0 and size & (size - 1) == 0


def suits(green_row, ta_count, ka_count):
    orbitals, local_rows, k_local = green_row.shape[1], green_row.shape[3], green_row.shape[4]
    return (
        ka_count == 2
        and orbitals * local_rows == SUBLANES
        and orbitals >= 4
        and halving(orbitals)
        and halving(ta_count)
        and ta_count % (2 * orbitals) == 0
        and k_local % LANES == 0
        and halving(k_local // LANES)
        and LANES % KS == 0
        and k_local * ka_count == KS * KS
    )


def fourier_tables(tiles):
    lane = np.arange(LANES)
    outer, inner = lane // KS, lane % KS
    group = LANES // KS
    angle = 2.0 * np.pi * (
        (outer[:, None] * outer[None, :] % group) / group + (inner[:, None] * inner[None, :] % KS) / KS
    )
    cosine, sine = np.cos(angle) / KS, np.sin(angle) / KS
    full = np.block([[cosine, sine], [-sine, cosine]]).astype(np.float32)
    high = full.astype(jnp.bfloat16)
    low = (full - high.astype(np.float32)).astype(jnp.bfloat16)
    turn = 2.0 * np.pi * (outer[None, :] * np.arange(tiles)[:, None]) / KS
    twiddle = np.stack([np.cos(turn), np.sin(turn)], axis=1).astype(np.float32)
    return jnp.asarray(np.stack([high, low])), jnp.asarray(twiddle)


def radix(values):
    count = len(values)
    if count == 1:
        return values
    half = count // 2
    sums, differences = [], []
    for place in range(half):
        (ar, ai), (br, bi) = values[place], values[place + half]
        sums.append((ar + br, ai + bi))
        dr, di = ar - br, ai - bi
        if place == 0:
            differences.append((dr, di))
        elif 4 * place == count:
            differences.append((-di, dr))
        else:
            cosine = math.cos(2.0 * math.pi * place / count)
            sine = math.sin(2.0 * math.pi * place / count)
            differences.append((dr * cosine - di * sine, dr * sine + di * cosine))
    even, odd = radix(sums), radix(differences)
    return [pair for both in zip(even, odd) for pair in both]


def turned(pair, twiddle_ref, tile):
    if tile == 0:
        return pair
    cosine, sine = twiddle_ref[tile, 0:1, :], twiddle_ref[tile, 1:2, :]
    return (pair[0] * cosine - pair[1] * sine, pair[0] * sine + pair[1] * cosine)


def lane_transform(rows, table_ref):
    high = rows.astype(jnp.bfloat16)
    low = (rows - high.astype(jnp.float32)).astype(jnp.bfloat16)
    first, second = table_ref[0], table_ref[1]
    dot = functools.partial(jnp.dot, preferred_element_type=jnp.float32)
    return dot(high, first) + (dot(low, first) + dot(high, second))


def to_sites(fields, table_ref, twiddle_ref):
    pieces = []
    for tiles in fields:
        for tile, pair in enumerate(radix(tiles)):
            pieces.append(jnp.concatenate(turned(pair, twiddle_ref, tile), axis=1))
    return lane_transform(jnp.concatenate(pieces, axis=0), table_ref)


def tiles_of(load, count):
    return [
        (load(0, pl.ds(tile * LANES, LANES)), load(1, pl.ds(tile * LANES, LANES)))
        for tile in range(count)
    ]


def emit_sigma(ka, space, screens_ref, table_ref, twiddle_ref, own_ref, send_ref):
    halves, k_local = own_ref.shape[2], own_ref.shape[4]
    local_tiles = k_local // LANES
    tiles = 2 * local_tiles
    green_real, green_imag = space[:, :LANES], space[:, LANES:]
    products = []
    for field in range(2):
        screen_real, screen_imag = screens_ref[field, :, :LANES], screens_ref[field, :, LANES:]
        real_part = -(green_real * screen_imag + green_imag * screen_real)
        conjugate = green_imag * screen_imag - green_real * screen_real
        products.append(jnp.concatenate([real_part, conjugate], axis=1))
    back = lane_transform(jnp.concatenate(products, axis=0), table_ref)
    for field in range(2):
        for half in range(halves):
            parts = []
            for tile in range(tiles):
                row = ((field * halves + half) * tiles + tile) * SUBLANES
                pair = (back[row : row + SUBLANES, :LANES], back[row : row + SUBLANES, LANES:])
                parts.append(turned(pair, twiddle_ref, tile))
            parts = radix(parts)
            for tile in range(local_tiles):
                for plane, sign in ((0, 1.0), (1, -1.0)):
                    near = (sign * parts[tile][plane]).astype(jnp.bfloat16).astype(jnp.float32)
                    far = (
                        (sign * parts[tile + local_tiles][plane])
                        .astype(jnp.bfloat16)
                        .astype(jnp.float32)
                    )
                    where_to = pl.ds(tile * LANES, LANES)
                    own_ref[field, plane, half, :, where_to] = jnp.where(ka == 0, near, far)
                    send_ref[field, plane, half, :, where_to] = jnp.where(ka == 0, far, near)


def opening_kernel(
    place_ref, own_ref, other_ref, table_ref, twiddle_ref, screens_ref, sigma_ref, send_ref
):
    halves, k_local = own_ref.shape[2], own_ref.shape[4]
    local_tiles = k_local // LANES
    spaces = []
    for field in range(3):
        rows = []
        for half in range(halves):
            near = tiles_of(lambda p, ds: own_ref[field, p, half, :, ds], local_tiles)
            far = tiles_of(lambda p, ds: other_ref[field, p, half, :, ds], local_tiles)
            rows.append(near + far)
        spaces.append(to_sites(rows, table_ref, twiddle_ref))
    screens_ref[0] = spaces[0]
    screens_ref[1] = spaces[1]
    emit_sigma(
        place_ref[1], spaces[2], screens_ref, table_ref, twiddle_ref, sigma_ref, send_ref
    )


def rate_pieces(own_side, ka, half, tile, onsite_ref, energy_ref, near_ref, far_ref, sums_refs):
    halves = near_ref.shape[1]
    lanes = pl.ds(tile * LANES, LANES)
    mine = ka if own_side else 1 - ka
    row = mine * halves + half
    here = near_ref if own_side else far_ref
    real_part = sums_refs[0][0, half, :, lanes] + sums_refs[1][0, half, :, lanes]
    imag_part = sums_refs[0][1, half, :, lanes] + sums_refs[1][1, half, :, lanes]
    energy = energy_ref[0:1, lanes]
    real_part = real_part + energy * here[0, half, :, lanes]
    imag_part = imag_part + energy * here[1, half, :, lanes]
    for side, ref in ((ka, near_ref), (1 - ka, far_ref)):
        for column in range(halves):
            coupling_real = onsite_ref[0, row, side * halves + column]
            coupling_imag = onsite_ref[1, row, side * halves + column]
            value_real, value_imag = ref[0, column, :, lanes], ref[1, column, :, lanes]
            real_part = real_part + coupling_real * value_real - coupling_imag * value_imag
            imag_part = imag_part + coupling_real * value_imag + coupling_imag * value_real
    return imag_part, -real_part


def advance_far_kernel(
    is_first, place_ref, onsite_ref, energy_ref, keep_ref, got_ref, near_ref, far_ref,
    green_ref, *refs
):
    ka = place_ref[1]
    if is_first:
        first_ref, estimate_ref = refs
    else:
        first_ref, estimate_ref = refs
    halves, k_local = far_ref.shape[1], far_ref.shape[3]
    for half in range(halves):
        for tile in range(k_local // LANES):
            lanes = pl.ds(tile * LANES, LANES)
            rates = rate_pieces(
                False, ka, half, tile, onsite_ref, energy_ref, near_ref, far_ref, (keep_ref, got_ref)
            )
            for plane in range(2):
                start = green_ref[plane, half, :, lanes]
                if is_first:
                    first_ref[plane, half, :, lanes] = rates[plane]
                    estimate_ref[plane, half, :, lanes] = start + time_step * rates[plane]
                else:
                    estimate_ref[plane, half, :, lanes] = start + 0.5 * time_step * (
                        first_ref[plane, half, :, lanes] + rates[plane]
                    )


def advance_near_kernel(
    is_first, place_ref, onsite_ref, energy_ref, keep_ref, got_ref, near_ref, far_ref,
    green_ref, arrived_ref, screens_ref, table_ref, twiddle_ref, *refs
):
    ka = place_ref[1]
    first_ref, estimate_ref, sigma_ref, send_ref = refs
    halves, k_local = near_ref.shape[1], near_ref.shape[3]
    local_tiles = k_local // LANES
    fields = []
    for half in range(halves):
        parts = []
        for tile in range(local_tiles):
            lanes = pl.ds(tile * LANES, LANES)
            rates = rate_pieces(
                True, ka, half, tile, onsite_ref, energy_ref, near_ref, far_ref, (keep_ref, got_ref)
            )
            pair = []
            for plane in range(2):
                start = green_ref[plane, half, :, lanes]
                if is_first:
                    first_ref[plane, half, :, lanes] = rates[plane]
                    value = start + time_step * rates[plane]
                else:
                    value = start + 0.5 * time_step * (
                        first_ref[plane, half, :, lanes] + rates[plane]
                    )
                estimate_ref[plane, half, :, lanes] = value
                pair.append(value)
            parts.append(tuple(pair))
        parts += tiles_of(lambda p, ds: arrived_ref[p, half, :, ds], local_tiles)
        fields.append(parts)
    space = to_sites(fields, table_ref, twiddle_ref)
    emit_sigma(ka, space, screens_ref, table_ref, twiddle_ref, sigma_ref, send_ref)


def closing_kernel(
    place_ref, onsite_ref, energy_ref, keep_near_ref, got_near_ref, keep_far_ref, got_far_ref,
    near_ref, far_ref, green_near_ref, green_far_ref, first_near_ref, first_far_ref,
    next_ref, latest_ref
):
    ka = place_ref[1]
    halves, k_local = near_ref.shape[1], near_ref.shape[3]
    sides = (
        (True, ka, (keep_near_ref, got_near_ref), green_near_ref, first_near_ref),
        (False, 1 - ka, (keep_far_ref, got_far_ref), green_far_ref, first_far_ref),
    )
    for own_side, side, sums_refs, green_ref, first_ref in sides:
        for half in range(halves):
            for tile in range(k_local // LANES):
                lanes = pl.ds(tile * LANES, LANES)
                rates = rate_pieces(
                    own_side, ka, half, tile, onsite_ref, energy_ref, near_ref, far_ref, sums_refs
                )
                for plane in range(2):
                    latest_ref[plane, side * halves + half, :, lanes] = rates[plane]
                    next_ref[plane, side * halves + half, :, lanes] = green_ref[
                        plane, half, :, lanes
                    ] + 0.5 * time_step * (first_ref[plane, half, :, lanes] + rates[plane])


def swap_rows(values, local_rows):
    count = len(values)
    group = lax.broadcasted_iota(jnp.int32, (SUBLANES, LANES), 0) // local_rows
    values = list(values)
    step = 1
    while step < count:
        low = (group & step) == 0
        for place in range(count):
            if place & step == 0:
                first, second = values[place], values[place | step]
                shift = step * local_rows
                values[place] = jnp.where(low, first, pltpu.roll(second, shift, 0))
                values[place | step] = jnp.where(
                    low, pltpu.roll(first, SUBLANES - shift, 0), second
                )
        step *= 2
    return values


def collide_kernel(
    order, times, place_ref, sigma_ref, causal_ref, lesser_ref, advanced_ref, keep_ref, send_ref
):
    halves = sigma_ref.shape[2]
    orbitals, local_rows, rows = lesser_ref.shape[1], lesser_ref.shape[3], lesser_ref.shape[4]
    me = place_ref[0]
    sums_real = [[None] * orbitals for _ in range(halves)]
    sums_imag = [[None] * orbitals for _ in range(halves)]

    def gather(total, value):
        return value if total is None else total + value

    for field, slab_ref in ((1, lesser_ref), (0, advanced_ref)):
        for stored in range(local_rows):
            for inner in range(orbitals):
                row = inner * local_rows + stored
                sigma_real, sigma_imag = [], []
                for half in range(halves):
                    for plane, found in ((0, sigma_real), (1, sigma_imag)):
                        value = sigma_ref[field, plane, half, row : row + 1, :]
                        value = jnp.broadcast_to(value, (rows, LANES))
                        if field == 0:
                            value = value * causal_ref[stored]
                        found.append(value)
                for outer in range(orbitals):
                    slab_real = slab_ref[0, inner, outer, stored].astype(jnp.float32)
                    slab_imag = slab_ref[1, inner, outer, stored].astype(jnp.float32)
                    for half in range(halves):
                        sums_real[half][outer] = (
                            gather(sums_real[half][outer], sigma_real[half] * slab_real)
                            - sigma_imag[half] * slab_imag
                        )
                        sums_imag[half][outer] = (
                            gather(sums_imag[half][outer], sigma_real[half] * slab_imag)
                            + sigma_imag[half] * slab_real
                        )
    first_tile = pl.program_id(1) * (rows // SUBLANES)
    for piece in range(rows // SUBLANES):
        for half in range(halves):
            for plane, sums in ((0, sums_real), (1, sums_imag)):
                begin = piece * SUBLANES
                owners = swap_rows(
                    [sums[half][outer][begin : begin + SUBLANES] for outer in range(orbitals)],
                    local_rows,
                )
                for pair in range(0, orbitals, 2):
                    relative = ((first_tile + piece) * orbitals + pair) ^ me
                    where_to = 0
                    for bit in order[1:]:
                        where_to = where_to * 2 + ((relative >> bit) & 1)
                    even = (me & 1) == 0
                    keep_ref[where_to, plane, half] = jnp.where(even, owners[pair], owners[pair + 1])
                    send_ref[where_to, plane, half] = jnp.where(even, owners[pair + 1], owners[pair])


def whole(memory_space=pltpu.VMEM):
    return pl.BlockSpec(memory_space=memory_space)


def float_like(*shape):
    return jax.ShapeDtypeStruct(shape, jnp.float32)


def flip(bit, count):
    return [(place, place ^ bit) for place in range(count)]


def halved_sum(keep, send, order, ta_count):
    got = lax.ppermute(send, "ta", flip(1 << order[0], ta_count))
    for bit in order[1:]:
        half = keep.shape[0] // 2
        outgoing = keep[half:] + got[half:]
        arriving = lax.ppermute(outgoing, "ta", flip(1 << bit, ta_count))
        keep, got = keep[:half] + got[:half], arriving
    return keep[0], got[0]


def fast(
    green_row, screen_lesser, screen_retarded, onsite, lesser_slab, advanced_slab, slab_start,
    block_table
):
    orbitals, local_rows, k_local = green_row.shape[1], green_row.shape[3], green_row.shape[4]
    ta_count, ka_count = lax.axis_size("ta"), lax.axis_size("ka")
    all_times = local_rows * ta_count
    halves = orbitals // 2
    tiles = k_local * ka_count // LANES
    ta_index, ka_index = lax.axis_index("ta"), lax.axis_index("ka")
    place = jnp.stack([ta_index, ka_index]).astype(jnp.int32)
    table, twiddle = fourier_tables(tiles)
    my_block = lax.dynamic_slice_in_dim(block_table, ta_index, 1)[0]
    row_times = my_block * local_rows + jnp.arange(local_rows, dtype=jnp.int32)
    col_times = jnp.repeat(block_table, local_rows) * local_rows + jnp.tile(
        jnp.arange(local_rows, dtype=jnp.int32), ta_count
    )
    causal = (row_times[:, None] <= col_times[None, :]).astype(jnp.float32)
    causal = jnp.broadcast_to(causal[:, :, None], (local_rows, all_times, LANES))
    momenta = ka_index * k_local + jnp.arange(k_local, dtype=jnp.int32)
    energy = dispersion(slab_start, all_times, momenta // KS, momenta % KS)[None]

    fields = jnp.stack([screen_lesser, screen_retarded, green_row])
    fields = fields.reshape(3, 2, orbitals, SUBLANES, k_local)
    near_fields = lax.dynamic_slice_in_dim(fields, ka_index * halves, halves, 2)
    far_fields = lax.dynamic_slice_in_dim(fields, (1 - ka_index) * halves, halves, 2)
    arrived_fields = lax.ppermute(far_fields, "ka", flip(1, ka_count))
    green_near, green_far = near_fields[2], far_fields[2]

    chunk = (2, halves, SUBLANES, k_local)
    scalar = whole(pltpu.SMEM)
    space_rows = halves * tiles * SUBLANES
    sigma_shape = float_like(2, *chunk)
    small = pltpu.CompilerParams(vmem_limit_bytes=16 * 1024 * 1024)

    screens, sigma_near, sigma_send = pl.pallas_call(
        opening_kernel,
        out_shape=(float_like(2, space_rows, 2 * LANES), sigma_shape, sigma_shape),
        in_specs=[scalar] + [whole()] * 4,
        out_specs=(whole(),) * 3,
        compiler_params=small,
        name="opening",
    )(place, near_fields, arrived_fields, table, twiddle)

    bits = ta_count.bit_length() - 1
    owner_bits = orbitals.bit_length() - 1
    low_bits, high_bits = list(range(1, owner_bits)), list(range(owner_bits, bits))
    orders = ([0] + low_bits + high_bits, [0] + high_bits + low_bits)
    rows = 2 * SUBLANES
    slab_spec = pl.BlockSpec(
        (2, orbitals, orbitals, local_rows, rows, LANES), lambda k, t: (0, 0, 0, 0, t, k)
    )
    halves_spec = pl.BlockSpec(
        (ta_count // 2, 2, halves, SUBLANES, LANES), lambda k, t: (0, 0, 0, 0, k)
    )

    def collide(sigma, order):
        return pl.pallas_call(
            functools.partial(collide_kernel, order, all_times),
            grid=(k_local // LANES, all_times // rows),
            out_shape=(float_like(ta_count // 2, *chunk),) * 2,
            in_specs=[
                scalar,
                pl.BlockSpec((2, 2, halves, SUBLANES, LANES), lambda k, t: (0, 0, 0, 0, k)),
                pl.BlockSpec((local_rows, rows, LANES), lambda k, t: (0, t, 0)),
                slab_spec,
                slab_spec,
            ],
            out_specs=(halves_spec, halves_spec),
            compiler_params=pltpu.CompilerParams(vmem_limit_bytes=16 * 1024 * 1024),
            cost_estimate=pl.CostEstimate(
                flops=16 * halves * orbitals * orbitals * local_rows * all_times * k_local,
                bytes_accessed=4 * lesser_slab.size,
                transcendentals=0,
            ),
            name="collide",
        )(place, sigma, causal, lesser_slab, advanced_slab)

    def collisions(sigma_near, sigma_send):
        sigma_far = lax.ppermute(sigma_send, "ka", flip(1, ka_count))
        near_sums = halved_sum(*collide(sigma_near, orders[0]), orders[0], ta_count)
        far_sums = halved_sum(*collide(sigma_far, orders[1]), orders[1], ta_count)
        return near_sums, far_sums

    estimate_near, estimate_far = green_near, green_far
    first_near = first_far = None
    for corrector in range(2):
        near_sums, far_sums = collisions(sigma_near, sigma_send)
        is_first = corrector == 0
        common = (place, onsite, energy)
        far_inputs = common + far_sums + (estimate_near, estimate_far, green_far)
        near_inputs = common + near_sums + (estimate_near, estimate_far, green_near)
        tables = (screens, table, twiddle)
        shape = float_like(*chunk)
        if is_first:
            far_out, near_out = (shape, shape), (shape, shape, sigma_shape, sigma_shape)
            extra_far, extra_near = (), ()
        else:
            far_out, near_out = (shape,), (shape, sigma_shape, sigma_shape)
            extra_far, extra_near = (first_far,), (first_near,)
        far_result = pl.pallas_call(
            functools.partial(advance_far_kernel, is_first),
            out_shape=far_out,
            in_specs=[scalar, scalar] + [whole()] * (6 + len(extra_far)),
            out_specs=(whole(),) * len(far_out),
            compiler_params=small,
            name="advance_far",
        )(*far_inputs, *extra_far)
        arrived = lax.ppermute(far_result[-1], "ka", flip(1, ka_count))
        near_result = pl.pallas_call(
            functools.partial(advance_near_kernel, is_first),
            out_shape=near_out,
            in_specs=[scalar, scalar] + [whole()] * (10 + len(extra_near)),
            out_specs=(whole(),) * len(near_out),
            compiler_params=small,
            name="advance_near",
        )(*near_inputs, arrived, *tables, *extra_near)
        if is_first:
            first_far, first_near = far_result[0], near_result[0]
        estimate_far = far_result[-1]
        estimate_near, sigma_near, sigma_send = near_result[-3:]
    near_sums, far_sums = collisions(sigma_near, sigma_send)
    full = float_like(2, orbitals, SUBLANES, k_local)
    next_row, latest = pl.pallas_call(
        closing_kernel,
        out_shape=(full, full),
        in_specs=[scalar, scalar] + [whole()] * 11,
        out_specs=(whole(), whole()),
        compiler_params=small,
        name="closing",
    )(
        place, onsite, energy, *near_sums, *far_sums, estimate_near, estimate_far, green_near,
        green_far, first_near, first_far,
    )
    return next_row.reshape(green_row.shape), latest.reshape(green_row.shape)

def local(*args):
    if suits(args[0], lax.axis_size("ta"), lax.axis_size("ka")):
        return fast(*args)
    return plain(*args)


def solution(mesh):
    return jax.shard_map(
        local,
        mesh=mesh,
        in_specs=(
            P(None, None, None, "ta", "ka"),
            P(None, None, None, "ta", "ka"),
            P(None, None, None, "ta", "ka"),
            P(),
            P(None, None, None, "ta", None, "ka"),
            P(None, None, None, "ta", None, "ka"),
            P(),
            P(),
        ),
        out_specs=(P(None, None, None, "ta", "ka"), P(None, None, None, "ta", "ka")),
        check_vma=False,
    )
```

```python
import functools
import math

import jax
import jax.numpy as jnp
import numpy as np
from jax import lax
from jax.experimental import pallas as pl
from jax.experimental.pallas import tpu as pltpu
from jax.sharding import PartitionSpec as P

KS = 32
LANES = 128
SUBLANES = 8


time_step = 0.1
drive_amp = 1.0
drive_freq = 0.37
highest = lax.Precision.HIGHEST


def phase_table(row_ids, col_ids, sign_value):
    products = row_ids[:, None] * col_ids[None, :] % KS
    angle = products.astype(jnp.float32) * (2.0 * math.pi / KS)
    factor = 1.0 / math.sqrt(KS)
    return (jnp.cos(angle) * factor, sign_value * jnp.sin(angle) * factor)


def along_last(values_in, cosine, sine_part):
    real_part = jnp.einsum("...m,mn->...n", values_in[0], cosine, precision=highest) - jnp.einsum(
        "...m,mn->...n", values_in[1], sine_part, precision=highest
    )
    imag_part = jnp.einsum(
        "...m,mn->...n", values_in[0], sine_part, precision=highest
    ) + jnp.einsum("...m,mn->...n", values_in[1], cosine, precision=highest)
    return jnp.stack([real_part, imag_part])


def along_second(values_in, cosine, sine_part):
    real_part = jnp.einsum("...mj,mn->...nj", values_in[0], cosine, precision=highest) - jnp.einsum(
        "...mj,mn->...nj", values_in[1], sine_part, precision=highest
    )
    imag_part = jnp.einsum(
        "...mj,mn->...nj", values_in[0], sine_part, precision=highest
    ) + jnp.einsum("...mj,mn->...nj", values_in[1], cosine, precision=highest)
    return jnp.stack([real_part, imag_part])


def transform(values_in, sign_value, ka_index):
    leading = values_in.shape[:-1]
    x_local = values_in.shape[-1] // KS
    numbers = jnp.arange(KS, dtype=jnp.int32)
    owned = ka_index * x_local + jnp.arange(x_local, dtype=jnp.int32)
    cosine, sine_part = phase_table(numbers, numbers, sign_value)
    partly = along_last(values_in.reshape(leading + (x_local, KS)), cosine, sine_part)
    gathered = lax.all_gather(partly.reshape(values_in.shape), "ka", axis=5, tiled=True)
    grid = gathered.reshape(leading + (KS, KS))
    col_cos, col_sin = phase_table(numbers, owned, sign_value)
    return along_second(grid, col_cos, col_sin).reshape(values_in.shape)


def self_energy(row_space, screens):
    green_real = row_space[0][None]
    green_imag = row_space[1][None]
    real_part = -(green_real * screens[1] + green_imag * screens[0])
    imag_part = green_real * screens[0] - green_imag * screens[1]
    return jnp.stack([real_part, imag_part])


def coupling(sigma_pair):
    return jnp.stack(
        [jnp.stack([sigma_pair[0], -sigma_pair[1]]), jnp.stack([sigma_pair[1], sigma_pair[0]])]
    )


def dispersion(slab_start, all_times, kx_ids, ky_ids):
    current = (slab_start[0] + all_times).astype(jnp.float32)
    shift = drive_amp * jnp.sin(drive_freq * current)
    factor = 2.0 * math.pi / KS
    return -2.0 * (
        jnp.cos(kx_ids.astype(jnp.float32) * factor + shift)
        + jnp.cos(ky_ids.astype(jnp.float32) * factor)
    )


def apply_h(row, onsite, energy):
    real_part = (
        jnp.einsum("ab,bctk->actk", onsite[0], row[0], precision=highest)
        - jnp.einsum("ab,bctk->actk", onsite[1], row[1], precision=highest)
        + energy * row[0]
    )
    imag_part = (
        jnp.einsum("ab,bctk->actk", onsite[0], row[1], precision=highest)
        + jnp.einsum("ab,bctk->actk", onsite[1], row[0], precision=highest)
        + energy * row[1]
    )
    return jnp.stack([real_part, imag_part])


def masked_product(less_coupling, row_times, piece_times, piece_adv):
    visible = row_times[:, None] <= piece_times[None, :]
    masked = jnp.where(visible[:, :, None], piece_adv, jnp.zeros_like(piece_adv))
    return jnp.einsum(
        "pqabsk,qbcstk->tpack", less_coupling, masked, preferred_element_type=jnp.float32
    )


def plain(
    green_row,
    screen_lesser,
    screen_retarded,
    onsite,
    lesser_slab,
    advanced_slab,
    slab_start,
    block_table,
):
    local_rows = green_row.shape[3]
    k_local = green_row.shape[4]
    ta_count = lax.axis_size("ta")
    all_times = local_rows * ta_count
    my_index = lax.axis_index("ta")
    ka_index = lax.axis_index("ka")
    my_block = lax.dynamic_slice_in_dim(block_table, my_index, 1)[0]
    row_times = my_block * local_rows + jnp.arange(local_rows, dtype=jnp.int32)
    col_times = jnp.repeat(block_table, local_rows) * local_rows + jnp.tile(
        jnp.arange(local_rows, dtype=jnp.int32), ta_count
    )
    momenta = ka_index * k_local + jnp.arange(k_local, dtype=jnp.int32)
    energy = dispersion(slab_start, all_times, momenta // KS, momenta % KS)
    first_space = transform(
        jnp.stack([screen_lesser, screen_retarded, green_row], axis=1), 1.0, ka_index
    )
    screens = first_space[:, 0:2]

    def rate_of(row, row_space):
        sigma_all = transform(self_energy(row_space, screens), -1.0, ka_index).astype(jnp.bfloat16)
        less_coupling = coupling(sigma_all[:, 0])
        ret_coupling = coupling(sigma_all[:, 1])
        totals = jnp.einsum(
            "pqabsk,qbcstk->tpack", ret_coupling, lesser_slab, preferred_element_type=jnp.float32
        )
        own_rows = lax.psum_scatter(
            totals + masked_product(less_coupling, row_times, col_times, advanced_slab),
            "ta",
            scatter_dimension=0,
            tiled=True,
        )
        collision = jnp.transpose(own_rows, (1, 2, 3, 0, 4))
        totals = apply_h(row, onsite, energy) + collision
        return jnp.stack([totals[1], -totals[0]])

    first_rate = rate_of(green_row, first_space[:, 2])
    estimate = green_row + time_step * first_rate
    latest = first_rate
    for _ in range(2):
        row_space = transform(estimate[:, None], 1.0, ka_index)[:, 0]
        latest = rate_of(estimate, row_space)
        estimate = green_row + 0.5 * time_step * (first_rate + latest)
    return (estimate, latest)


def halving(size):
    return size > 0 and size & (size - 1) == 0


def suits(green_row, ta_count, ka_count):
    orbitals, local_rows, k_local = green_row.shape[1], green_row.shape[3], green_row.shape[4]
    return (
        ka_count == 2
        and orbitals * local_rows == SUBLANES
        and orbitals >= 4
        and halving(orbitals)
        and halving(ta_count)
        and ta_count % (2 * orbitals) == 0
        and k_local % LANES == 0
        and halving(k_local // LANES)
        and LANES % KS == 0
        and k_local * ka_count == KS * KS
    )


def fourier_tables(tiles):
    lane = np.arange(LANES)
    outer, inner = lane // KS, lane % KS
    group = LANES // KS
    angle = 2.0 * np.pi * (
        (outer[:, None] * outer[None, :] % group) / group + (inner[:, None] * inner[None, :] % KS) / KS
    )
    cosine, sine = np.cos(angle) / KS, np.sin(angle) / KS
    full = np.block([[cosine, sine], [-sine, cosine]]).astype(np.float32)
    high = full.astype(jnp.bfloat16)
    low = (full - high.astype(np.float32)).astype(jnp.bfloat16)
    turn = 2.0 * np.pi * (outer[None, :] * np.arange(tiles)[:, None]) / KS
    twiddle = np.stack([np.cos(turn), np.sin(turn)], axis=1).astype(np.float32)
    return jnp.asarray(np.stack([high, low])), jnp.asarray(twiddle)


def radix(values):
    count = len(values)
    if count == 1:
        return values
    half = count // 2
    sums, differences = [], []
    for place in range(half):
        (ar, ai), (br, bi) = values[place], values[place + half]
        sums.append((ar + br, ai + bi))
        dr, di = ar - br, ai - bi
        if place == 0:
            differences.append((dr, di))
        elif 4 * place == count:
            differences.append((-di, dr))
        else:
            cosine = math.cos(2.0 * math.pi * place / count)
            sine = math.sin(2.0 * math.pi * place / count)
            differences.append((dr * cosine - di * sine, dr * sine + di * cosine))
    even, odd = radix(sums), radix(differences)
    return [pair for both in zip(even, odd) for pair in both]


def turned(pair, twiddle_ref, tile):
    if tile == 0:
        return pair
    cosine, sine = twiddle_ref[tile, 0:1, :], twiddle_ref[tile, 1:2, :]
    return (pair[0] * cosine - pair[1] * sine, pair[0] * sine + pair[1] * cosine)


def lane_transform(rows, table_ref):
    high = rows.astype(jnp.bfloat16)
    low = (rows - high.astype(jnp.float32)).astype(jnp.bfloat16)
    first, second = table_ref[0], table_ref[1]
    dot = functools.partial(jnp.dot, preferred_element_type=jnp.float32)
    return dot(high, first) + (dot(low, first) + dot(high, second))


def to_sites(fields, table_ref, twiddle_ref):
    pieces = []
    for tiles in fields:
        for tile, pair in enumerate(radix(tiles)):
            pieces.append(jnp.concatenate(turned(pair, twiddle_ref, tile), axis=1))
    return lane_transform(jnp.concatenate(pieces, axis=0), table_ref)


def tiles_of(load, count):
    return [
        (load(0, pl.ds(tile * LANES, LANES)), load(1, pl.ds(tile * LANES, LANES)))
        for tile in range(count)
    ]


def emit_sigma(ka, space, screens_ref, table_ref, twiddle_ref, own_ref, send_ref):
    halves, k_local = own_ref.shape[2], own_ref.shape[4]
    local_tiles = k_local // LANES
    tiles = 2 * local_tiles
    green_real, green_imag = space[:, :LANES], space[:, LANES:]
    products = []
    for field in range(2):
        screen_real, screen_imag = screens_ref[field, :, :LANES], screens_ref[field, :, LANES:]
        real_part = -(green_real * screen_imag + green_imag * screen_real)
        conjugate = green_imag * screen_imag - green_real * screen_real
        products.append(jnp.concatenate([real_part, conjugate], axis=1))
    back = lane_transform(jnp.concatenate(products, axis=0), table_ref)
    for field in range(2):
        for half in range(halves):
            parts = []
            for tile in range(tiles):
                row = ((field * halves + half) * tiles + tile) * SUBLANES
                pair = (back[row : row + SUBLANES, :LANES], back[row : row + SUBLANES, LANES:])
                parts.append(turned(pair, twiddle_ref, tile))
            parts = radix(parts)
            for tile in range(local_tiles):
                for plane, sign in ((0, 1.0), (1, -1.0)):
                    near = (sign * parts[tile][plane]).astype(jnp.bfloat16).astype(jnp.float32)
                    far = (
                        (sign * parts[tile + local_tiles][plane])
                        .astype(jnp.bfloat16)
                        .astype(jnp.float32)
                    )
                    where_to = pl.ds(tile * LANES, LANES)
                    own_ref[field, plane, half, :, where_to] = jnp.where(ka == 0, near, far)
                    send_ref[field, plane, half, :, where_to] = jnp.where(ka == 0, far, near)


def pack_kernel(own_side, place_ref, lesser_ref, retarded_ref, green_ref, packed_ref):
    halves, inner, local_rows = packed_ref.shape[2], lesser_ref.shape[2], lesser_ref.shape[3]
    side = place_ref[1] if own_side else 1 - place_ref[1]
    for field, ref in enumerate((lesser_ref, retarded_ref, green_ref)):
        for plane in range(2):
            for half in range(halves):
                for column in range(inner):
                    begin = column * local_rows
                    packed_ref[field, plane, half, begin : begin + local_rows, :] = ref[
                        plane, side * halves + half, column
                    ]


def opening_kernel(
    place_ref, own_ref, other_ref, table_ref, twiddle_ref, screens_ref, sigma_ref, send_ref
):
    halves, k_local = own_ref.shape[2], own_ref.shape[4]
    local_tiles = k_local // LANES
    spaces = []
    for field in range(3):
        rows = []
        for half in range(halves):
            near = tiles_of(lambda p, ds: own_ref[field, p, half, :, ds], local_tiles)
            far = tiles_of(lambda p, ds: other_ref[field, p, half, :, ds], local_tiles)
            rows.append(near + far)
        spaces.append(to_sites(rows, table_ref, twiddle_ref))
    screens_ref[0] = spaces[0]
    screens_ref[1] = spaces[1]
    emit_sigma(
        place_ref[1], spaces[2], screens_ref, table_ref, twiddle_ref, sigma_ref, send_ref
    )


def rate_pieces(own_side, ka, half, tile, onsite_ref, energy_ref, near_ref, far_ref, sums_refs):
    halves = near_ref.shape[1]
    lanes = pl.ds(tile * LANES, LANES)
    mine = ka if own_side else 1 - ka
    row = mine * halves + half
    here = near_ref if own_side else far_ref
    real_part = functools.reduce(jnp.add, [ref[0, half, :, lanes] for ref in sums_refs])
    imag_part = functools.reduce(jnp.add, [ref[1, half, :, lanes] for ref in sums_refs])
    energy = energy_ref[0:1, lanes]
    real_part = real_part + energy * here[0, half, :, lanes]
    imag_part = imag_part + energy * here[1, half, :, lanes]
    for side, ref in ((ka, near_ref), (1 - ka, far_ref)):
        for column in range(halves):
            coupling_real = onsite_ref[0, row, side * halves + column]
            coupling_imag = onsite_ref[1, row, side * halves + column]
            value_real, value_imag = ref[0, column, :, lanes], ref[1, column, :, lanes]
            real_part = real_part + coupling_real * value_real - coupling_imag * value_imag
            imag_part = imag_part + coupling_real * value_imag + coupling_imag * value_real
    return imag_part, -real_part


def advance_far_kernel(
    is_first, sums_count, place_ref, onsite_ref, energy_ref, near_ref, far_ref, green_ref, *refs
):
    ka = place_ref[1]
    sums_refs, (first_ref, estimate_ref) = refs[:sums_count], refs[sums_count:]
    halves, k_local = far_ref.shape[1], far_ref.shape[3]
    for half in range(halves):
        for tile in range(k_local // LANES):
            lanes = pl.ds(tile * LANES, LANES)
            rates = rate_pieces(
                False, ka, half, tile, onsite_ref, energy_ref, near_ref, far_ref, sums_refs
            )
            for plane in range(2):
                start = green_ref[plane, half, :, lanes]
                if is_first:
                    first_ref[plane, half, :, lanes] = rates[plane]
                    estimate_ref[plane, half, :, lanes] = start + time_step * rates[plane]
                else:
                    estimate_ref[plane, half, :, lanes] = start + 0.5 * time_step * (
                        first_ref[plane, half, :, lanes] + rates[plane]
                    )


def advance_near_kernel(
    is_first, sums_count, place_ref, onsite_ref, energy_ref, near_ref, far_ref, green_ref,
    arrived_ref, screens_ref, table_ref, twiddle_ref, *refs
):
    ka = place_ref[1]
    sums_refs = refs[:sums_count]
    first_ref, estimate_ref, sigma_ref, send_ref = refs[sums_count:]
    halves, k_local = near_ref.shape[1], near_ref.shape[3]
    local_tiles = k_local // LANES
    fields = []
    for half in range(halves):
        parts = []
        for tile in range(local_tiles):
            lanes = pl.ds(tile * LANES, LANES)
            rates = rate_pieces(
                True, ka, half, tile, onsite_ref, energy_ref, near_ref, far_ref, sums_refs
            )
            pair = []
            for plane in range(2):
                start = green_ref[plane, half, :, lanes]
                if is_first:
                    first_ref[plane, half, :, lanes] = rates[plane]
                    value = start + time_step * rates[plane]
                else:
                    value = start + 0.5 * time_step * (
                        first_ref[plane, half, :, lanes] + rates[plane]
                    )
                estimate_ref[plane, half, :, lanes] = value
                pair.append(value)
            parts.append(tuple(pair))
        parts += tiles_of(lambda p, ds: arrived_ref[p, half, :, ds], local_tiles)
        fields.append(parts)
    space = to_sites(fields, table_ref, twiddle_ref)
    emit_sigma(ka, space, screens_ref, table_ref, twiddle_ref, sigma_ref, send_ref)


def closing_kernel(
    near_count, far_count, place_ref, onsite_ref, energy_ref, near_ref, far_ref, green_near_ref,
    green_far_ref, first_near_ref, first_far_ref, *refs
):
    ka = place_ref[1]
    near_sums, far_sums = refs[:near_count], refs[near_count : near_count + far_count]
    next_ref, latest_ref = refs[near_count + far_count :]
    halves, k_local = near_ref.shape[1], near_ref.shape[3]
    sides = (
        (True, ka, near_sums, green_near_ref, first_near_ref),
        (False, 1 - ka, far_sums, green_far_ref, first_far_ref),
    )
    for own_side, side, sums_refs, green_ref, first_ref in sides:
        for half in range(halves):
            for tile in range(k_local // LANES):
                lanes = pl.ds(tile * LANES, LANES)
                rates = rate_pieces(
                    own_side, ka, half, tile, onsite_ref, energy_ref, near_ref, far_ref, sums_refs
                )
                for plane in range(2):
                    value = green_ref[plane, half, :, lanes] + 0.5 * time_step * (
                        first_ref[plane, half, :, lanes] + rates[plane]
                    )
                    for column in range(next_ref.shape[2]):
                        begin = column * next_ref.shape[3]
                        span = slice(begin, begin + next_ref.shape[3])
                        latest_ref[plane, side * halves + half, column, :, lanes] = rates[plane][span]
                        next_ref[plane, side * halves + half, column, :, lanes] = value[span]


def swap_rows(values, local_rows):
    count = len(values)
    group = lax.broadcasted_iota(jnp.int32, (SUBLANES, LANES), 0) // local_rows
    values = list(values)
    step = 1
    while step < count:
        low = (group & step) == 0
        for place in range(count):
            if place & step == 0:
                first, second = values[place], values[place | step]
                shift = step * local_rows
                values[place] = jnp.where(low, first, pltpu.roll(second, shift, 0))
                values[place | step] = jnp.where(
                    low, pltpu.roll(first, SUBLANES - shift, 0), second
                )
        step *= 2
    return values


def collide_kernel(
    order, place_ref, sigma_ref, causal_ref, lesser_ref, advanced_ref, keep_ref, send_ref
):
    halves, k_local = sigma_ref.shape[2], sigma_ref.shape[4]
    orbitals, local_rows, times = lesser_ref.shape[1], lesser_ref.shape[3], lesser_ref.shape[4]
    rows = 2 * SUBLANES
    time_steps = times // rows
    me = place_ref[0]

    def gather(total, value):
        return value if total is None else total + value

    def step(counter, carried):
        time_step_index = counter % time_steps
        first_row = pl.multiple_of(time_step_index * rows, rows)
        lanes = pl.ds(pl.multiple_of(counter // time_steps * LANES, LANES), LANES)
        here = pl.ds(first_row, rows)
        sums_real = [[None] * orbitals for _ in range(halves)]
        sums_imag = [[None] * orbitals for _ in range(halves)]
        for field, slab_ref in ((1, lesser_ref), (0, advanced_ref)):
            for stored in range(local_rows):
                for inner in range(orbitals):
                    row = inner * local_rows + stored
                    sigma_real, sigma_imag = [], []
                    for half in range(halves):
                        for plane, found in ((0, sigma_real), (1, sigma_imag)):
                            value = sigma_ref[field, plane, half, row : row + 1, lanes]
                            value = jnp.broadcast_to(value, (rows, LANES))
                            if field == 0:
                                value = value * causal_ref[stored, here]
                            found.append(value)
                    for outer in range(orbitals):
                        slab_real = slab_ref[0, inner, outer, stored, here, lanes]
                        slab_imag = slab_ref[1, inner, outer, stored, here, lanes]
                        slab_real = slab_real.astype(jnp.float32)
                        slab_imag = slab_imag.astype(jnp.float32)
                        for half in range(halves):
                            sums_real[half][outer] = (
                                gather(sums_real[half][outer], sigma_real[half] * slab_real)
                                - sigma_imag[half] * slab_imag
                            )
                            sums_imag[half][outer] = (
                                gather(sums_imag[half][outer], sigma_real[half] * slab_imag)
                                + sigma_imag[half] * slab_real
                            )
        even = (me & 1) == 0
        for piece in range(rows // SUBLANES):
            tile = time_step_index * (rows // SUBLANES) + piece
            begin = piece * SUBLANES
            for half in range(halves):
                for plane, sums in ((0, sums_real), (1, sums_imag)):
                    owners = swap_rows(
                        [sums[half][outer][begin : begin + SUBLANES] for outer in range(orbitals)],
                        local_rows,
                    )
                    for pair in range(0, orbitals, 2):
                        relative = (tile * orbitals + pair) ^ me
                        where_to = 0
                        for bit in order[1:]:
                            where_to = where_to * 2 + ((relative >> bit) & 1)
                        first, second = owners[pair], owners[pair + 1]
                        keep_ref[where_to, plane, half, :, lanes] = jnp.where(even, first, second)
                        send_ref[where_to, plane, half, :, lanes] = jnp.where(even, second, first)
        return carried

    lax.fori_loop(0, time_steps * (k_local // LANES), step, 0)


def whole(memory_space=pltpu.VMEM):
    return pl.BlockSpec(memory_space=memory_space)


def float_like(*shape):
    return jax.ShapeDtypeStruct(shape, jnp.float32)


def flip(bit, count):
    return [(place, place ^ bit) for place in range(count)]


def halved_sum(keep, send, order, direct_bits, ta_count):
    got = lax.ppermute(send, "ta", flip(1 << order[0], ta_count))
    for bit in order[1 : len(order) - direct_bits]:
        half = keep.shape[0] // 2
        outgoing = keep[half:] + got[half:]
        arriving = lax.ppermute(outgoing, "ta", flip(1 << bit, ta_count))
        keep, got = keep[:half] + got[:half], arriving
    if direct_bits == 0:
        return keep[0], got[0]
    shift = order[-1]
    pieces = [keep[place] + got[place] for place in range(1 << direct_bits)]
    results = []
    for place in range(1, 1 << direct_bits):
        results.append(lax.ppermute(pieces[place], "ta", flip(place << shift, ta_count)))
    return (pieces[0], *results)


def fast(
    green_row, screen_lesser, screen_retarded, onsite, lesser_slab, advanced_slab, slab_start,
    block_table
):
    orbitals, local_rows, k_local = green_row.shape[1], green_row.shape[3], green_row.shape[4]
    ta_count, ka_count = lax.axis_size("ta"), lax.axis_size("ka")
    all_times = local_rows * ta_count
    halves = orbitals // 2
    tiles = k_local * ka_count // LANES
    ta_index, ka_index = lax.axis_index("ta"), lax.axis_index("ka")
    place = jnp.stack([ta_index, ka_index]).astype(jnp.int32)
    table, twiddle = fourier_tables(tiles)
    my_block = lax.dynamic_slice_in_dim(block_table, ta_index, 1)[0]
    row_times = my_block * local_rows + jnp.arange(local_rows, dtype=jnp.int32)
    col_times = jnp.repeat(block_table, local_rows) * local_rows + jnp.tile(
        jnp.arange(local_rows, dtype=jnp.int32), ta_count
    )
    causal = (row_times[:, None] <= col_times[None, :]).astype(jnp.float32)
    causal = jnp.broadcast_to(causal[:, :, None], (local_rows, all_times, LANES))
    momenta = ka_index * k_local + jnp.arange(k_local, dtype=jnp.int32)
    energy = dispersion(slab_start, all_times, momenta // KS, momenta % KS)[None]

    chunk = (2, halves, SUBLANES, k_local)
    scalar = whole(pltpu.SMEM)
    space_rows = halves * tiles * SUBLANES
    sigma_shape = float_like(2, *chunk)
    small = pltpu.CompilerParams(vmem_limit_bytes=8 * 1024 * 1024)

    def packed(own_side):
        return pl.pallas_call(
            functools.partial(pack_kernel, own_side),
            out_shape=float_like(3, *chunk),
            in_specs=[scalar] + [whole()] * 3,
            out_specs=whole(),
            compiler_params=small,
            name="pack",
        )(place, screen_lesser, screen_retarded, green_row)

    far_fields = packed(False)
    arrived_fields = lax.ppermute(far_fields, "ka", flip(1, ka_count))
    near_fields = packed(True)
    green_near, green_far = near_fields[2], far_fields[2]

    screens, sigma_near, sigma_send = pl.pallas_call(
        opening_kernel,
        out_shape=(float_like(2, space_rows, 2 * LANES), sigma_shape, sigma_shape),
        in_specs=[scalar] + [whole()] * 4,
        out_specs=(whole(),) * 3,
        compiler_params=small,
        name="opening",
    )(place, near_fields, arrived_fields, table, twiddle)

    bits = ta_count.bit_length() - 1
    owner_bits = orbitals.bit_length() - 1
    order = list(range(owner_bits)) + list(range(owner_bits, bits))[::-1]
    direct_bits = bits - owner_bits

    def collide(sigma):
        return pl.pallas_call(
            functools.partial(collide_kernel, order),
            out_shape=(float_like(ta_count // 2, *chunk),) * 2,
            in_specs=[scalar] + [whole()] * 4,
            out_specs=(whole(),) * 2,
            compiler_params=small,
            cost_estimate=pl.CostEstimate(
                flops=16 * halves * orbitals * orbitals * local_rows * all_times * k_local,
                bytes_accessed=4 * lesser_slab.size,
                transcendentals=0,
            ),
            name="collide",
        )(place, sigma, causal, lesser_slab, advanced_slab)

    def collisions(sigma_near, sigma_send):
        sigma_far = lax.ppermute(sigma_send, "ka", flip(1, ka_count))
        near = collide(sigma_near)
        far = collide(sigma_far)
        near_sums = halved_sum(*near, order, 0, ta_count)
        far_sums = halved_sum(*far, order, direct_bits, ta_count)
        return near_sums, far_sums

    estimate_near, estimate_far = green_near, green_far
    first_near = first_far = None
    chunk_shape = float_like(*chunk)
    for corrector in range(2):
        near_sums, far_sums = collisions(sigma_near, sigma_send)
        is_first = corrector == 0
        common = (place, onsite, energy, estimate_near, estimate_far)
        tables = (screens, table, twiddle)
        if is_first:
            far_out, near_out = (chunk_shape,) * 2, (chunk_shape,) * 2
            extra_far, extra_near = (), ()
        else:
            far_out, near_out = (chunk_shape,), (chunk_shape,)
            extra_far, extra_near = (first_far,), (first_near,)
        near_out = near_out + (sigma_shape,) * 2
        far_inputs = common + (green_far,) + far_sums + extra_far
        far_result = pl.pallas_call(
            functools.partial(advance_far_kernel, is_first, len(far_sums)),
            out_shape=far_out,
            in_specs=[scalar, scalar] + [whole()] * (len(far_inputs) - 2),
            out_specs=(whole(),) * len(far_out),
            compiler_params=small,
            name="advance_far",
        )(*far_inputs)
        arrived = lax.ppermute(far_result[-1], "ka", flip(1, ka_count))
        near_inputs = common + (green_near, arrived) + tables + near_sums + extra_near
        near_result = pl.pallas_call(
            functools.partial(advance_near_kernel, is_first, len(near_sums)),
            out_shape=near_out,
            in_specs=[scalar, scalar] + [whole()] * (len(near_inputs) - 2),
            out_specs=(whole(),) * len(near_out),
            compiler_params=small,
            name="advance_near",
        )(*near_inputs)
        if is_first:
            first_far, first_near = far_result[0], near_result[0]
        estimate_far = far_result[-1]
        estimate_near, sigma_near, sigma_send = near_result[-3:]
    near_sums, far_sums = collisions(sigma_near, sigma_send)
    full = float_like(*green_row.shape)
    return pl.pallas_call(
        functools.partial(closing_kernel, len(near_sums), len(far_sums)),
        out_shape=(full, full),
        in_specs=[scalar, scalar] + [whole()] * (7 + len(near_sums) + len(far_sums)),
        out_specs=(whole(), whole()),
        compiler_params=small,
        name="closing",
    )(
        place, onsite, energy, estimate_near, estimate_far, green_near, green_far, first_near,
        first_far, *near_sums, *far_sums,
    )


def local(*args):
    if suits(args[0], lax.axis_size("ta"), lax.axis_size("ka")):
        return fast(*args)
    return plain(*args)


def solution(mesh):
    return jax.shard_map(
        local,
        mesh=mesh,
        in_specs=(
            P(None, None, None, "ta", "ka"),
            P(None, None, None, "ta", "ka"),
            P(None, None, None, "ta", "ka"),
            P(),
            P(None, None, None, "ta", None, "ka"),
            P(None, None, None, "ta", None, "ka"),
            P(),
            P(),
        ),
        out_specs=(P(None, None, None, "ta", "ka"), P(None, None, None, "ta", "ka")),
        check_vma=False,
    )
```

```python
import functools
import math

import jax
import jax.numpy as jnp
import numpy as np
from jax import lax
from jax.experimental import pallas as pl
from jax.experimental.pallas import tpu as pltpu
from jax.sharding import PartitionSpec as P

KS = 32
LANES = 128
SUBLANES = 8


time_step = 0.1
drive_amp = 1.0
drive_freq = 0.37
highest = lax.Precision.HIGHEST


def phase_table(row_ids, col_ids, sign_value):
    products = row_ids[:, None] * col_ids[None, :] % KS
    angle = products.astype(jnp.float32) * (2.0 * math.pi / KS)
    factor = 1.0 / math.sqrt(KS)
    return (jnp.cos(angle) * factor, sign_value * jnp.sin(angle) * factor)


def along_last(values_in, cosine, sine_part):
    real_part = jnp.einsum("...m,mn->...n", values_in[0], cosine, precision=highest) - jnp.einsum(
        "...m,mn->...n", values_in[1], sine_part, precision=highest
    )
    imag_part = jnp.einsum(
        "...m,mn->...n", values_in[0], sine_part, precision=highest
    ) + jnp.einsum("...m,mn->...n", values_in[1], cosine, precision=highest)
    return jnp.stack([real_part, imag_part])


def along_second(values_in, cosine, sine_part):
    real_part = jnp.einsum("...mj,mn->...nj", values_in[0], cosine, precision=highest) - jnp.einsum(
        "...mj,mn->...nj", values_in[1], sine_part, precision=highest
    )
    imag_part = jnp.einsum(
        "...mj,mn->...nj", values_in[0], sine_part, precision=highest
    ) + jnp.einsum("...mj,mn->...nj", values_in[1], cosine, precision=highest)
    return jnp.stack([real_part, imag_part])


def transform(values_in, sign_value, ka_index):
    leading = values_in.shape[:-1]
    x_local = values_in.shape[-1] // KS
    numbers = jnp.arange(KS, dtype=jnp.int32)
    owned = ka_index * x_local + jnp.arange(x_local, dtype=jnp.int32)
    cosine, sine_part = phase_table(numbers, numbers, sign_value)
    partly = along_last(values_in.reshape(leading + (x_local, KS)), cosine, sine_part)
    gathered = lax.all_gather(partly.reshape(values_in.shape), "ka", axis=5, tiled=True)
    grid = gathered.reshape(leading + (KS, KS))
    col_cos, col_sin = phase_table(numbers, owned, sign_value)
    return along_second(grid, col_cos, col_sin).reshape(values_in.shape)


def self_energy(row_space, screens):
    green_real = row_space[0][None]
    green_imag = row_space[1][None]
    real_part = -(green_real * screens[1] + green_imag * screens[0])
    imag_part = green_real * screens[0] - green_imag * screens[1]
    return jnp.stack([real_part, imag_part])


def coupling(sigma_pair):
    return jnp.stack(
        [jnp.stack([sigma_pair[0], -sigma_pair[1]]), jnp.stack([sigma_pair[1], sigma_pair[0]])]
    )


def dispersion(slab_start, all_times, kx_ids, ky_ids):
    current = (slab_start[0] + all_times).astype(jnp.float32)
    shift = drive_amp * jnp.sin(drive_freq * current)
    factor = 2.0 * math.pi / KS
    return -2.0 * (
        jnp.cos(kx_ids.astype(jnp.float32) * factor + shift)
        + jnp.cos(ky_ids.astype(jnp.float32) * factor)
    )


def apply_h(row, onsite, energy):
    real_part = (
        jnp.einsum("ab,bctk->actk", onsite[0], row[0], precision=highest)
        - jnp.einsum("ab,bctk->actk", onsite[1], row[1], precision=highest)
        + energy * row[0]
    )
    imag_part = (
        jnp.einsum("ab,bctk->actk", onsite[0], row[1], precision=highest)
        + jnp.einsum("ab,bctk->actk", onsite[1], row[0], precision=highest)
        + energy * row[1]
    )
    return jnp.stack([real_part, imag_part])


def masked_product(less_coupling, row_times, piece_times, piece_adv):
    visible = row_times[:, None] <= piece_times[None, :]
    masked = jnp.where(visible[:, :, None], piece_adv, jnp.zeros_like(piece_adv))
    return jnp.einsum(
        "pqabsk,qbcstk->tpack", less_coupling, masked, preferred_element_type=jnp.float32
    )


def plain(
    green_row,
    screen_lesser,
    screen_retarded,
    onsite,
    lesser_slab,
    advanced_slab,
    slab_start,
    block_table,
):
    local_rows = green_row.shape[3]
    k_local = green_row.shape[4]
    ta_count = lax.axis_size("ta")
    all_times = local_rows * ta_count
    my_index = lax.axis_index("ta")
    ka_index = lax.axis_index("ka")
    my_block = lax.dynamic_slice_in_dim(block_table, my_index, 1)[0]
    row_times = my_block * local_rows + jnp.arange(local_rows, dtype=jnp.int32)
    col_times = jnp.repeat(block_table, local_rows) * local_rows + jnp.tile(
        jnp.arange(local_rows, dtype=jnp.int32), ta_count
    )
    momenta = ka_index * k_local + jnp.arange(k_local, dtype=jnp.int32)
    energy = dispersion(slab_start, all_times, momenta // KS, momenta % KS)
    first_space = transform(
        jnp.stack([screen_lesser, screen_retarded, green_row], axis=1), 1.0, ka_index
    )
    screens = first_space[:, 0:2]

    def rate_of(row, row_space):
        sigma_all = transform(self_energy(row_space, screens), -1.0, ka_index).astype(jnp.bfloat16)
        less_coupling = coupling(sigma_all[:, 0])
        ret_coupling = coupling(sigma_all[:, 1])
        totals = jnp.einsum(
            "pqabsk,qbcstk->tpack", ret_coupling, lesser_slab, preferred_element_type=jnp.float32
        )
        own_rows = lax.psum_scatter(
            totals + masked_product(less_coupling, row_times, col_times, advanced_slab),
            "ta",
            scatter_dimension=0,
            tiled=True,
        )
        collision = jnp.transpose(own_rows, (1, 2, 3, 0, 4))
        totals = apply_h(row, onsite, energy) + collision
        return jnp.stack([totals[1], -totals[0]])

    first_rate = rate_of(green_row, first_space[:, 2])
    estimate = green_row + time_step * first_rate
    latest = first_rate
    for _ in range(2):
        row_space = transform(estimate[:, None], 1.0, ka_index)[:, 0]
        latest = rate_of(estimate, row_space)
        estimate = green_row + 0.5 * time_step * (first_rate + latest)
    return (estimate, latest)


def halving(size):
    return size > 0 and size & (size - 1) == 0


def suits(green_row, ta_count, ka_count):
    orbitals, local_rows, k_local = green_row.shape[1], green_row.shape[3], green_row.shape[4]
    return (
        ka_count == 2
        and orbitals * local_rows == SUBLANES
        and orbitals >= 4
        and halving(orbitals)
        and halving(ta_count)
        and ta_count % (2 * orbitals) == 0
        and k_local % LANES == 0
        and halving(k_local // LANES)
        and LANES % KS == 0
        and k_local * ka_count == KS * KS
    )


def fourier_tables(tiles):
    lane = np.arange(LANES)
    outer, inner = lane // KS, lane % KS
    group = LANES // KS
    angle = 2.0 * np.pi * (
        (outer[:, None] * outer[None, :] % group) / group + (inner[:, None] * inner[None, :] % KS) / KS
    )
    cosine, sine = np.cos(angle) / KS, np.sin(angle) / KS
    full = np.block([[cosine, sine], [-sine, cosine]]).astype(np.float32)
    high = full.astype(jnp.bfloat16)
    low = (full - high.astype(np.float32)).astype(jnp.bfloat16)
    turn = 2.0 * np.pi * (outer[None, :] * np.arange(tiles)[:, None]) / KS
    twiddle = np.stack([np.cos(turn), np.sin(turn)], axis=1).astype(np.float32)
    return jnp.asarray(np.stack([high, low])), jnp.asarray(twiddle)


def radix(values):
    count = len(values)
    if count == 1:
        return values
    half = count // 2
    sums, differences = [], []
    for place in range(half):
        (ar, ai), (br, bi) = values[place], values[place + half]
        sums.append((ar + br, ai + bi))
        dr, di = ar - br, ai - bi
        if place == 0:
            differences.append((dr, di))
        elif 4 * place == count:
            differences.append((-di, dr))
        else:
            cosine = math.cos(2.0 * math.pi * place / count)
            sine = math.sin(2.0 * math.pi * place / count)
            differences.append((dr * cosine - di * sine, dr * sine + di * cosine))
    even, odd = radix(sums), radix(differences)
    return [pair for both in zip(even, odd) for pair in both]


def turned(pair, twiddle_ref, tile):
    if tile == 0:
        return pair
    cosine, sine = twiddle_ref[tile, 0:1, :], twiddle_ref[tile, 1:2, :]
    return (pair[0] * cosine - pair[1] * sine, pair[0] * sine + pair[1] * cosine)


def lane_transform(rows, table_ref):
    high = rows.astype(jnp.bfloat16)
    low = (rows - high.astype(jnp.float32)).astype(jnp.bfloat16)
    first, second = table_ref[0], table_ref[1]
    dot = functools.partial(jnp.dot, preferred_element_type=jnp.float32)
    return dot(high, first) + (dot(low, first) + dot(high, second))


def to_sites(fields, table_ref, twiddle_ref):
    pieces = []
    for tiles in fields:
        for tile, pair in enumerate(radix(tiles)):
            pieces.append(jnp.concatenate(turned(pair, twiddle_ref, tile), axis=1))
    return lane_transform(jnp.concatenate(pieces, axis=0), table_ref)


def tiles_of(load, count):
    return [
        (load(0, pl.ds(tile * LANES, LANES)), load(1, pl.ds(tile * LANES, LANES)))
        for tile in range(count)
    ]


def emit_sigma(ka, space, screens_ref, table_ref, twiddle_ref, own_ref, send_ref):
    halves, k_local = own_ref.shape[2], own_ref.shape[4]
    local_tiles = k_local // LANES
    tiles = 2 * local_tiles
    green_real, green_imag = space[:, :LANES], space[:, LANES:]
    products = []
    for field in range(2):
        screen_real, screen_imag = screens_ref[field, :, :LANES], screens_ref[field, :, LANES:]
        real_part = -(green_real * screen_imag + green_imag * screen_real)
        conjugate = green_imag * screen_imag - green_real * screen_real
        products.append(jnp.concatenate([real_part, conjugate], axis=1))
    back = lane_transform(jnp.concatenate(products, axis=0), table_ref)
    for field in range(2):
        for half in range(halves):
            parts = []
            for tile in range(tiles):
                row = ((field * halves + half) * tiles + tile) * SUBLANES
                pair = (back[row : row + SUBLANES, :LANES], back[row : row + SUBLANES, LANES:])
                parts.append(turned(pair, twiddle_ref, tile))
            parts = radix(parts)
            for tile in range(local_tiles):
                for plane, sign in ((0, 1.0), (1, -1.0)):
                    near = (sign * parts[tile][plane]).astype(jnp.bfloat16).astype(jnp.float32)
                    far = (
                        (sign * parts[tile + local_tiles][plane])
                        .astype(jnp.bfloat16)
                        .astype(jnp.float32)
                    )
                    where_to = pl.ds(tile * LANES, LANES)
                    own_ref[field, plane, half, :, where_to] = jnp.where(ka == 0, near, far)
                    send_ref[field, plane, half, :, where_to] = jnp.where(ka == 0, far, near)


def pack_kernel(lesser_ref, retarded_ref, green_ref, near_ref, far_ref):
    ka = lax.axis_index("ka")
    halves, inner, local_rows = near_ref.shape[2], lesser_ref.shape[2], lesser_ref.shape[3]
    for side, packed_ref in ((1 - ka, far_ref), (ka, near_ref)):
        for field, ref in enumerate((lesser_ref, retarded_ref, green_ref)):
            for plane in range(2):
                for half in range(halves):
                    for column in range(inner):
                        begin = column * local_rows
                        packed_ref[field, plane, half, begin : begin + local_rows, :] = ref[
                            plane, side * halves + half, column
                        ]


def stage_kernel(
    blocks_ref, onsite_ref, energies_ref, table_in_ref, twiddle_in_ref,
    causal_ref, energy_ref, onsite_out_ref, table_ref, twiddle_ref
):
    ta, ka = lax.axis_index("ta"), lax.axis_index("ka")
    table_ref[...] = table_in_ref[...]
    twiddle_ref[...] = twiddle_in_ref[...]
    local_rows, all_times, k_local = causal_ref.shape[0], causal_ref.shape[1], energy_ref.shape[1]
    energy_ref[...] = energies_ref[:, pl.ds(pl.multiple_of(ka * k_local, LANES), k_local)]
    orbitals = onsite_ref.shape[1]
    halves = orbitals // 2
    for row in range(orbitals):
        for column in range(orbitals):
            for plane in range(2):
                value = onsite_ref[
                    plane, (row + ka * halves) % orbitals, (column + ka * halves) % orbitals
                ]
                place = (plane * orbitals + row) * orbitals + column
                onsite_out_ref[place : place + 1, :] = jnp.full((1, LANES), value)
    for stored in range(local_rows):
        row_time = blocks_ref[ta] * local_rows + stored
        for column in range(all_times):
            column_time = blocks_ref[column // local_rows] * local_rows + column % local_rows
            seen = jnp.where(row_time <= column_time, jnp.float32(1.0), jnp.float32(0.0))
            causal_ref[stored, column : column + 1, :] = jnp.full((1, LANES), seen)


def opening_kernel(
    own_ref, other_ref, table_ref, twiddle_ref, screens_ref, sigma_ref, send_ref
):
    halves, k_local = own_ref.shape[2], own_ref.shape[4]
    local_tiles = k_local // LANES
    spaces = []
    for field in range(3):
        rows = []
        for half in range(halves):
            near = tiles_of(lambda p, ds: own_ref[field, p, half, :, ds], local_tiles)
            far = tiles_of(lambda p, ds: other_ref[field, p, half, :, ds], local_tiles)
            rows.append(near + far)
        spaces.append(to_sites(rows, table_ref, twiddle_ref))
    screens_ref[0] = spaces[0]
    screens_ref[1] = spaces[1]
    emit_sigma(
        lax.axis_index("ka"), spaces[2], screens_ref, table_ref, twiddle_ref, sigma_ref, send_ref
    )


def rate_pieces(own_side, half, tile, onsite_ref, energy_ref, near_ref, far_ref, sums_refs):
    halves = near_ref.shape[1]
    orbitals = 2 * halves
    lanes = pl.ds(tile * LANES, LANES)
    row = half if own_side else halves + half
    here = near_ref if own_side else far_ref
    real_part = functools.reduce(jnp.add, [ref[0, half, :, lanes] for ref in sums_refs])
    imag_part = functools.reduce(jnp.add, [ref[1, half, :, lanes] for ref in sums_refs])
    energy = energy_ref[0:1, lanes]
    real_part = real_part + energy * here[0, half, :, lanes]
    imag_part = imag_part + energy * here[1, half, :, lanes]
    for side, ref in enumerate((near_ref, far_ref)):
        for column in range(halves):
            place = row * orbitals + side * halves + column
            coupling_real = onsite_ref[place : place + 1, :]
            place += orbitals * orbitals
            coupling_imag = onsite_ref[place : place + 1, :]
            value_real, value_imag = ref[0, column, :, lanes], ref[1, column, :, lanes]
            real_part = real_part + coupling_real * value_real - coupling_imag * value_imag
            imag_part = imag_part + coupling_real * value_imag + coupling_imag * value_real
    return imag_part, -real_part


def advance_far_kernel(
    is_first, sums_count, onsite_ref, energy_ref, near_ref, far_ref, green_ref, *refs
):
    sums_refs, (first_ref, estimate_ref) = refs[:sums_count], refs[sums_count:]
    halves, k_local = far_ref.shape[1], far_ref.shape[3]
    for half in range(halves):
        for tile in range(k_local // LANES):
            lanes = pl.ds(tile * LANES, LANES)
            rates = rate_pieces(
                False, half, tile, onsite_ref, energy_ref, near_ref, far_ref, sums_refs
            )
            for plane in range(2):
                start = green_ref[plane, half, :, lanes]
                if is_first:
                    first_ref[plane, half, :, lanes] = rates[plane]
                    estimate_ref[plane, half, :, lanes] = start + time_step * rates[plane]
                else:
                    estimate_ref[plane, half, :, lanes] = start + 0.5 * time_step * (
                        first_ref[plane, half, :, lanes] + rates[plane]
                    )


def advance_near_kernel(
    is_first, sums_count, onsite_ref, energy_ref, near_ref, far_ref, green_ref,
    arrived_ref, screens_ref, table_ref, twiddle_ref, *refs
):
    ka = lax.axis_index("ka")
    sums_refs = refs[:sums_count]
    first_ref, estimate_ref, sigma_ref, send_ref = refs[sums_count:]
    halves, k_local = near_ref.shape[1], near_ref.shape[3]
    local_tiles = k_local // LANES
    fields = []
    for half in range(halves):
        parts = []
        for tile in range(local_tiles):
            lanes = pl.ds(tile * LANES, LANES)
            rates = rate_pieces(
                True, half, tile, onsite_ref, energy_ref, near_ref, far_ref, sums_refs
            )
            pair = []
            for plane in range(2):
                start = green_ref[plane, half, :, lanes]
                if is_first:
                    first_ref[plane, half, :, lanes] = rates[plane]
                    value = start + time_step * rates[plane]
                else:
                    value = start + 0.5 * time_step * (
                        first_ref[plane, half, :, lanes] + rates[plane]
                    )
                estimate_ref[plane, half, :, lanes] = value
                pair.append(value)
            parts.append(tuple(pair))
        parts += tiles_of(lambda p, ds: arrived_ref[p, half, :, ds], local_tiles)
        fields.append(parts)
    space = to_sites(fields, table_ref, twiddle_ref)
    emit_sigma(ka, space, screens_ref, table_ref, twiddle_ref, sigma_ref, send_ref)


def closing_kernel(
    near_count, far_count, onsite_ref, energy_ref, near_ref, far_ref, green_near_ref,
    green_far_ref, first_near_ref, first_far_ref, *refs
):
    ka = lax.axis_index("ka")
    near_sums, far_sums = refs[:near_count], refs[near_count : near_count + far_count]
    next_ref, latest_ref = refs[near_count + far_count :]
    halves, k_local = near_ref.shape[1], near_ref.shape[3]
    sides = (
        (True, ka, near_sums, green_near_ref, first_near_ref),
        (False, 1 - ka, far_sums, green_far_ref, first_far_ref),
    )
    for own_side, side, sums_refs, green_ref, first_ref in sides:
        for half in range(halves):
            for tile in range(k_local // LANES):
                lanes = pl.ds(tile * LANES, LANES)
                rates = rate_pieces(
                    own_side, half, tile, onsite_ref, energy_ref, near_ref, far_ref, sums_refs
                )
                for plane in range(2):
                    value = green_ref[plane, half, :, lanes] + 0.5 * time_step * (
                        first_ref[plane, half, :, lanes] + rates[plane]
                    )
                    for column in range(next_ref.shape[2]):
                        begin = column * next_ref.shape[3]
                        span = slice(begin, begin + next_ref.shape[3])
                        latest_ref[plane, side * halves + half, column, :, lanes] = rates[plane][span]
                        next_ref[plane, side * halves + half, column, :, lanes] = value[span]


def swap_rows(values, local_rows):
    count = len(values)
    group = lax.broadcasted_iota(jnp.int32, (SUBLANES, LANES), 0) // local_rows
    values = list(values)
    step = 1
    while step < count:
        low = (group & step) == 0
        for place in range(count):
            if place & step == 0:
                first, second = values[place], values[place | step]
                shift = step * local_rows
                values[place] = jnp.where(low, first, pltpu.roll(second, shift, 0))
                values[place | step] = jnp.where(
                    low, pltpu.roll(first, SUBLANES - shift, 0), second
                )
        step *= 2
    return values


def collide_kernel(
    order, sigma_ref, causal_ref, lesser_ref, advanced_ref, keep_ref, send_ref
):
    halves, k_local = sigma_ref.shape[2], sigma_ref.shape[4]
    orbitals, local_rows, times = lesser_ref.shape[1], lesser_ref.shape[3], lesser_ref.shape[4]
    rows = SUBLANES
    time_steps = times // rows
    me = lax.axis_index("ta")

    def gather(total, value):
        return value if total is None else total + value

    def step(counter, carried):
        tile = counter % time_steps
        here = pl.ds(pl.multiple_of(tile * rows, rows), rows)
        lanes = pl.ds(pl.multiple_of(counter // time_steps * LANES, LANES), LANES)
        sums = [[[None] * 3 for _ in range(orbitals)] for _ in range(halves)]
        for field, slab_ref in ((1, lesser_ref), (0, advanced_ref)):
            for stored in range(local_rows):
                for inner in range(orbitals):
                    row = inner * local_rows + stored
                    sigmas = []
                    for half in range(halves):
                        triple = [
                            jnp.broadcast_to(
                                sigma_ref[field, plane, half, row : row + 1, lanes], (rows, LANES)
                            )
                            for plane in range(2)
                        ]
                        if field == 0:
                            triple = [value * causal_ref[stored, here] for value in triple]
                        sigmas.append(triple + [triple[0] + triple[1]])
                    for outer in range(orbitals):
                        slabs = [
                            slab_ref[plane, inner, outer, stored, here, lanes].astype(jnp.float32)
                            for plane in range(2)
                        ]
                        slabs.append(slabs[0] + slabs[1])
                        for half in range(halves):
                            totals = sums[half][outer]
                            for term in range(3):
                                totals[term] = gather(
                                    totals[term], sigmas[half][term] * slabs[term]
                                )
        even = (me & 1) == 0
        for half in range(halves):
            real_parts = [totals[0] - totals[1] for totals in sums[half]]
            imag_parts = [totals[2] - (totals[0] + totals[1]) for totals in sums[half]]
            for plane, parts in ((0, real_parts), (1, imag_parts)):
                owners = swap_rows(parts, local_rows)
                for pair in range(0, orbitals, 2):
                    relative = (tile * orbitals + pair) ^ me
                    where_to = 0
                    for bit in order[1:]:
                        where_to = where_to * 2 + ((relative >> bit) & 1)
                    first, second = owners[pair], owners[pair + 1]
                    keep_ref[where_to, plane, half, :, lanes] = jnp.where(even, first, second)
                    send_ref[where_to, plane, half, :, lanes] = jnp.where(even, second, first)
        return carried

    lax.fori_loop(0, time_steps * (k_local // LANES), step, 0)


def whole(memory_space=pltpu.VMEM):
    return pl.BlockSpec(memory_space=memory_space)


def float_like(*shape):
    return jax.ShapeDtypeStruct(shape, jnp.float32)


def flip(bit, count):
    return [(place, place ^ bit) for place in range(count)]


def halved_sum(keep, send, order, direct_bits, ta_count):
    got = lax.ppermute(send, "ta", flip(1 << order[0], ta_count))
    for bit in order[1 : len(order) - direct_bits]:
        half = keep.shape[0] // 2
        outgoing = keep[half:] + got[half:]
        arriving = lax.ppermute(outgoing, "ta", flip(1 << bit, ta_count))
        keep, got = keep[:half] + got[:half], arriving
    if direct_bits == 0:
        return keep[0], got[0]
    shift = order[-1]
    pieces = [keep[place] + got[place] for place in range(1 << direct_bits)]
    results = []
    for place in range(1, 1 << direct_bits):
        results.append(lax.ppermute(pieces[place], "ta", flip(place << shift, ta_count)))
    return (pieces[0], *results)


def fast(
    green_row, screen_lesser, screen_retarded, onsite, lesser_slab, advanced_slab, slab_start,
    block_table
):
    orbitals, local_rows, k_local = green_row.shape[1], green_row.shape[3], green_row.shape[4]
    ta_count, ka_count = lax.axis_size("ta"), lax.axis_size("ka")
    all_times = local_rows * ta_count
    halves = orbitals // 2
    tiles = k_local * ka_count // LANES
    table, twiddle = fourier_tables(tiles)
    momenta = jnp.arange(KS * KS, dtype=jnp.int32)
    start = lax.optimization_barrier(jnp.broadcast_to(slab_start, momenta.shape))
    energies = dispersion(start[None], all_times, momenta // KS, momenta % KS)[None]

    chunk = (2, halves, SUBLANES, k_local)
    scalar = whole(pltpu.SMEM)
    space_rows = halves * tiles * SUBLANES
    sigma_shape = float_like(2, *chunk)
    small = pltpu.CompilerParams(vmem_limit_bytes=8 * 1024 * 1024)

    hint = pl.CostEstimate(
        flops=8 * lesser_slab.size, bytes_accessed=8 * lesser_slab.size, transcendentals=0
    )
    near_fields, far_fields = pl.pallas_call(
        pack_kernel,
        out_shape=(float_like(3, *chunk),) * 2,
        in_specs=[whole()] * 3,
        out_specs=(whole(),) * 2,
        compiler_params=small,
        cost_estimate=hint,
        name="pack",
    )(screen_lesser, screen_retarded, green_row)
    arrived_fields = lax.ppermute(far_fields, "ka", flip(1, ka_count))
    causal, energy, onsite, table, twiddle = pl.pallas_call(
        stage_kernel,
        out_shape=(
            float_like(local_rows, all_times, LANES),
            float_like(1, k_local),
            float_like(2 * orbitals * orbitals, LANES),
            jax.ShapeDtypeStruct(table.shape, table.dtype),
            jax.ShapeDtypeStruct(twiddle.shape, twiddle.dtype),
        ),
        in_specs=[scalar] * 2 + [whole()] * 3,
        out_specs=(whole(),) * 5,
        compiler_params=small,
        cost_estimate=hint,
        name="stage",
    )(block_table, onsite, energies, table, twiddle)
    green_near, green_far = near_fields[2], far_fields[2]

    screens, sigma_near, sigma_send = pl.pallas_call(
        opening_kernel,
        out_shape=(float_like(2, space_rows, 2 * LANES), sigma_shape, sigma_shape),
        in_specs=[whole()] * 4,
        out_specs=(whole(),) * 3,
        compiler_params=small,
        cost_estimate=hint,
        name="opening",
    )(near_fields, arrived_fields, table, twiddle)

    bits = ta_count.bit_length() - 1
    owner_bits = orbitals.bit_length() - 1
    near_order = list(range(bits))
    far_order = list(range(owner_bits)) + list(range(owner_bits, bits))[::-1]
    direct_bits = bits - owner_bits

    def collide(sigma, order):
        return pl.pallas_call(
            functools.partial(collide_kernel, order),
            out_shape=(float_like(ta_count // 2, *chunk),) * 2,
            in_specs=[whole()] * 4,
            out_specs=(whole(),) * 2,
            compiler_params=small,
            cost_estimate=pl.CostEstimate(
                flops=16 * halves * orbitals * orbitals * local_rows * all_times * k_local,
                bytes_accessed=4 * lesser_slab.size,
                transcendentals=0,
            ),
            name="collide",
        )(sigma, causal, lesser_slab, advanced_slab)

    def collisions(sigma_near, sigma_send):
        sigma_far = lax.ppermute(sigma_send, "ka", flip(1, ka_count))
        near = collide(sigma_near, near_order)
        far = collide(sigma_far, far_order)
        near_sums = halved_sum(*near, near_order, 0, ta_count)
        far_sums = halved_sum(*far, far_order, direct_bits, ta_count)
        return near_sums, far_sums

    estimate_near, estimate_far = green_near, green_far
    first_near = first_far = None
    chunk_shape = float_like(*chunk)
    for corrector in range(2):
        is_first = corrector == 0
        near_sums, far_sums = collisions(sigma_near, sigma_send)
        common = (onsite, energy, estimate_near, estimate_far)
        tables = (screens, table, twiddle)
        if is_first:
            far_out, near_out = (chunk_shape,) * 2, (chunk_shape,) * 2
            extra_far, extra_near = (), ()
        else:
            far_out, near_out = (chunk_shape,), (chunk_shape,)
            extra_far, extra_near = (first_far,), (first_near,)
        near_out = near_out + (sigma_shape,) * 2
        far_inputs = common + (green_far,) + far_sums + extra_far
        far_result = pl.pallas_call(
            functools.partial(advance_far_kernel, is_first, len(far_sums)),
            out_shape=far_out,
            in_specs=[whole()] * len(far_inputs),
            out_specs=(whole(),) * len(far_out),
            compiler_params=small,
            name="advance_far",
        )(*far_inputs)
        arrived = lax.ppermute(far_result[-1], "ka", flip(1, ka_count))
        near_inputs = common + (green_near, arrived) + tables + near_sums + extra_near
        near_result = pl.pallas_call(
            functools.partial(advance_near_kernel, is_first, len(near_sums)),
            out_shape=near_out,
            in_specs=[whole()] * len(near_inputs),
            out_specs=(whole(),) * len(near_out),
            compiler_params=small,
            name="advance_near",
        )(*near_inputs)
        if is_first:
            first_far, first_near = far_result[0], near_result[0]
        estimate_far = far_result[-1]
        estimate_near, sigma_near, sigma_send = near_result[-3:]
    near_sums, far_sums = collisions(sigma_near, sigma_send)
    full = float_like(*green_row.shape)
    return pl.pallas_call(
        functools.partial(closing_kernel, len(near_sums), len(far_sums)),
        out_shape=(full, full),
        in_specs=[whole()] * (8 + len(near_sums) + len(far_sums)),
        out_specs=(whole(), whole()),
        compiler_params=small,
        name="closing",
    )(
        onsite, energy, estimate_near, estimate_far, green_near, green_far, first_near,
        first_far, *near_sums, *far_sums,
    )


def local(*args):
    if suits(args[0], lax.axis_size("ta"), lax.axis_size("ka")):
        return fast(*args)
    return plain(*args)


def solution(mesh):
    return jax.shard_map(
        local,
        mesh=mesh,
        in_specs=(
            P(None, None, None, "ta", "ka"),
            P(None, None, None, "ta", "ka"),
            P(None, None, None, "ta", "ka"),
            P(),
            P(None, None, None, "ta", None, "ka"),
            P(None, None, None, "ta", None, "ka"),
            P(),
            P(),
        ),
        out_specs=(P(None, None, None, "ta", "ka"), P(None, None, None, "ta", "ka")),
        check_vma=False,
    )
```

```python
import functools
import math

import jax
import jax.numpy as jnp
import numpy as np
from jax import lax
from jax.experimental import pallas as pl
from jax.experimental.pallas import tpu as pltpu
from jax.sharding import PartitionSpec as P

KS = 32
LANES = 128
SUBLANES = 8


time_step = 0.1
drive_amp = 1.0
drive_freq = 0.37
highest = lax.Precision.HIGHEST


def phase_table(row_ids, col_ids, sign_value):
    products = row_ids[:, None] * col_ids[None, :] % KS
    angle = products.astype(jnp.float32) * (2.0 * math.pi / KS)
    factor = 1.0 / math.sqrt(KS)
    return (jnp.cos(angle) * factor, sign_value * jnp.sin(angle) * factor)


def along_last(values_in, cosine, sine_part):
    real_part = jnp.einsum("...m,mn->...n", values_in[0], cosine, precision=highest) - jnp.einsum(
        "...m,mn->...n", values_in[1], sine_part, precision=highest
    )
    imag_part = jnp.einsum(
        "...m,mn->...n", values_in[0], sine_part, precision=highest
    ) + jnp.einsum("...m,mn->...n", values_in[1], cosine, precision=highest)
    return jnp.stack([real_part, imag_part])


def along_second(values_in, cosine, sine_part):
    real_part = jnp.einsum("...mj,mn->...nj", values_in[0], cosine, precision=highest) - jnp.einsum(
        "...mj,mn->...nj", values_in[1], sine_part, precision=highest
    )
    imag_part = jnp.einsum(
        "...mj,mn->...nj", values_in[0], sine_part, precision=highest
    ) + jnp.einsum("...mj,mn->...nj", values_in[1], cosine, precision=highest)
    return jnp.stack([real_part, imag_part])


def transform(values_in, sign_value, ka_index):
    leading = values_in.shape[:-1]
    x_local = values_in.shape[-1] // KS
    numbers = jnp.arange(KS, dtype=jnp.int32)
    owned = ka_index * x_local + jnp.arange(x_local, dtype=jnp.int32)
    cosine, sine_part = phase_table(numbers, numbers, sign_value)
    partly = along_last(values_in.reshape(leading + (x_local, KS)), cosine, sine_part)
    gathered = lax.all_gather(partly.reshape(values_in.shape), "ka", axis=5, tiled=True)
    grid = gathered.reshape(leading + (KS, KS))
    col_cos, col_sin = phase_table(numbers, owned, sign_value)
    return along_second(grid, col_cos, col_sin).reshape(values_in.shape)


def self_energy(row_space, screens):
    green_real = row_space[0][None]
    green_imag = row_space[1][None]
    real_part = -(green_real * screens[1] + green_imag * screens[0])
    imag_part = green_real * screens[0] - green_imag * screens[1]
    return jnp.stack([real_part, imag_part])


def coupling(sigma_pair):
    return jnp.stack(
        [jnp.stack([sigma_pair[0], -sigma_pair[1]]), jnp.stack([sigma_pair[1], sigma_pair[0]])]
    )


def dispersion(slab_start, all_times, kx_ids, ky_ids):
    current = (slab_start[0] + all_times).astype(jnp.float32)
    shift = drive_amp * jnp.sin(drive_freq * current)
    factor = 2.0 * math.pi / KS
    return -2.0 * (
        jnp.cos(kx_ids.astype(jnp.float32) * factor + shift)
        + jnp.cos(ky_ids.astype(jnp.float32) * factor)
    )


def apply_h(row, onsite, energy):
    real_part = (
        jnp.einsum("ab,bctk->actk", onsite[0], row[0], precision=highest)
        - jnp.einsum("ab,bctk->actk", onsite[1], row[1], precision=highest)
        + energy * row[0]
    )
    imag_part = (
        jnp.einsum("ab,bctk->actk", onsite[0], row[1], precision=highest)
        + jnp.einsum("ab,bctk->actk", onsite[1], row[0], precision=highest)
        + energy * row[1]
    )
    return jnp.stack([real_part, imag_part])


def masked_product(less_coupling, row_times, piece_times, piece_adv):
    visible = row_times[:, None] <= piece_times[None, :]
    masked = jnp.where(visible[:, :, None], piece_adv, jnp.zeros_like(piece_adv))
    return jnp.einsum(
        "pqabsk,qbcstk->tpack", less_coupling, masked, preferred_element_type=jnp.float32
    )


def plain(
    green_row,
    screen_lesser,
    screen_retarded,
    onsite,
    lesser_slab,
    advanced_slab,
    slab_start,
    block_table,
):
    local_rows = green_row.shape[3]
    k_local = green_row.shape[4]
    ta_count = lax.axis_size("ta")
    all_times = local_rows * ta_count
    my_index = lax.axis_index("ta")
    ka_index = lax.axis_index("ka")
    my_block = lax.dynamic_slice_in_dim(block_table, my_index, 1)[0]
    row_times = my_block * local_rows + jnp.arange(local_rows, dtype=jnp.int32)
    col_times = jnp.repeat(block_table, local_rows) * local_rows + jnp.tile(
        jnp.arange(local_rows, dtype=jnp.int32), ta_count
    )
    momenta = ka_index * k_local + jnp.arange(k_local, dtype=jnp.int32)
    energy = dispersion(slab_start, all_times, momenta // KS, momenta % KS)
    first_space = transform(
        jnp.stack([screen_lesser, screen_retarded, green_row], axis=1), 1.0, ka_index
    )
    screens = first_space[:, 0:2]

    def rate_of(row, row_space):
        sigma_all = transform(self_energy(row_space, screens), -1.0, ka_index).astype(jnp.bfloat16)
        less_coupling = coupling(sigma_all[:, 0])
        ret_coupling = coupling(sigma_all[:, 1])
        totals = jnp.einsum(
            "pqabsk,qbcstk->tpack", ret_coupling, lesser_slab, preferred_element_type=jnp.float32
        )
        own_rows = lax.psum_scatter(
            totals + masked_product(less_coupling, row_times, col_times, advanced_slab),
            "ta",
            scatter_dimension=0,
            tiled=True,
        )
        collision = jnp.transpose(own_rows, (1, 2, 3, 0, 4))
        totals = apply_h(row, onsite, energy) + collision
        return jnp.stack([totals[1], -totals[0]])

    first_rate = rate_of(green_row, first_space[:, 2])
    estimate = green_row + time_step * first_rate
    latest = first_rate
    for _ in range(2):
        row_space = transform(estimate[:, None], 1.0, ka_index)[:, 0]
        latest = rate_of(estimate, row_space)
        estimate = green_row + 0.5 * time_step * (first_rate + latest)
    return (estimate, latest)


def halving(size):
    return size > 0 and size & (size - 1) == 0


def suits(green_row, ta_count, ka_count):
    orbitals, local_rows, k_local = green_row.shape[1], green_row.shape[3], green_row.shape[4]
    return (
        ka_count == 2
        and orbitals * local_rows == SUBLANES
        and orbitals >= 4
        and halving(orbitals)
        and halving(ta_count)
        and ta_count % (2 * orbitals) == 0
        and k_local % LANES == 0
        and halving(k_local // LANES)
        and LANES % KS == 0
        and k_local * ka_count == KS * KS
    )


def fourier_tables(tiles):
    lane = np.arange(LANES)
    outer, inner = lane // KS, lane % KS
    group = LANES // KS
    angle = 2.0 * np.pi * (
        (outer[:, None] * outer[None, :] % group) / group + (inner[:, None] * inner[None, :] % KS) / KS
    )
    cosine, sine = np.cos(angle) / KS, np.sin(angle) / KS
    full = np.block([[cosine, sine], [-sine, cosine]]).astype(np.float32)
    high = full.astype(jnp.bfloat16)
    low = (full - high.astype(np.float32)).astype(jnp.bfloat16)
    turn = 2.0 * np.pi * (outer[None, :] * np.arange(tiles)[:, None]) / KS
    twiddle = np.stack([np.cos(turn), np.sin(turn)], axis=1).astype(np.float32)
    return jnp.asarray(np.stack([high, low])), jnp.asarray(twiddle)


def radix(values):
    count = len(values)
    if count == 1:
        return values
    half = count // 2
    sums, differences = [], []
    for place in range(half):
        (ar, ai), (br, bi) = values[place], values[place + half]
        sums.append((ar + br, ai + bi))
        dr, di = ar - br, ai - bi
        if place == 0:
            differences.append((dr, di))
        elif 4 * place == count:
            differences.append((-di, dr))
        else:
            cosine = math.cos(2.0 * math.pi * place / count)
            sine = math.sin(2.0 * math.pi * place / count)
            differences.append((dr * cosine - di * sine, dr * sine + di * cosine))
    even, odd = radix(sums), radix(differences)
    return [pair for both in zip(even, odd) for pair in both]


def turned(pair, twiddle_ref, tile):
    if tile == 0:
        return pair
    cosine, sine = twiddle_ref[tile, 0:1, :], twiddle_ref[tile, 1:2, :]
    return (pair[0] * cosine - pair[1] * sine, pair[0] * sine + pair[1] * cosine)


def lane_transform(rows, table_ref):
    high = rows.astype(jnp.bfloat16)
    low = (rows - high.astype(jnp.float32)).astype(jnp.bfloat16)
    first, second = table_ref[0], table_ref[1]
    dot = functools.partial(jnp.dot, preferred_element_type=jnp.float32)
    return dot(high, first) + (dot(low, first) + dot(high, second))


def to_sites(fields, table_ref, twiddle_ref):
    pieces = []
    for tiles in fields:
        for tile, pair in enumerate(radix(tiles)):
            pieces.append(jnp.concatenate(turned(pair, twiddle_ref, tile), axis=1))
    return lane_transform(jnp.concatenate(pieces, axis=0), table_ref)


def tiles_of(load, count):
    return [
        (load(0, pl.ds(tile * LANES, LANES)), load(1, pl.ds(tile * LANES, LANES)))
        for tile in range(count)
    ]


def emit_sigma(ka, space, screens_ref, table_ref, twiddle_ref, own_ref, send_ref):
    halves, k_local = own_ref.shape[2], own_ref.shape[4]
    local_tiles = k_local // LANES
    tiles = 2 * local_tiles
    green_real, green_imag = space[:, :LANES], space[:, LANES:]
    products = []
    for field in range(2):
        screen_real, screen_imag = screens_ref[field, :, :LANES], screens_ref[field, :, LANES:]
        real_part = -(green_real * screen_imag + green_imag * screen_real)
        conjugate = green_imag * screen_imag - green_real * screen_real
        products.append(jnp.concatenate([real_part, conjugate], axis=1))
    back = lane_transform(jnp.concatenate(products, axis=0), table_ref)
    for field in range(2):
        for half in range(halves):
            parts = []
            for tile in range(tiles):
                row = ((field * halves + half) * tiles + tile) * SUBLANES
                pair = (back[row : row + SUBLANES, :LANES], back[row : row + SUBLANES, LANES:])
                parts.append(turned(pair, twiddle_ref, tile))
            parts = radix(parts)
            for tile in range(local_tiles):
                for plane, sign in ((0, 1.0), (1, -1.0)):
                    near = (sign * parts[tile][plane]).astype(jnp.bfloat16).astype(jnp.float32)
                    far = (
                        (sign * parts[tile + local_tiles][plane])
                        .astype(jnp.bfloat16)
                        .astype(jnp.float32)
                    )
                    where_to = pl.ds(tile * LANES, LANES)
                    own_ref[field, plane, half, :, where_to] = jnp.where(ka == 0, near, far)
                    send_ref[field, plane, half, :, where_to] = jnp.where(ka == 0, far, near)


def pack_kernel(lesser_ref, retarded_ref, green_ref, near_ref, far_ref):
    ka = lax.axis_index("ka")
    halves, inner, local_rows = near_ref.shape[2], lesser_ref.shape[2], lesser_ref.shape[3]
    for side, packed_ref in ((1 - ka, far_ref), (ka, near_ref)):
        for field, ref in enumerate((lesser_ref, retarded_ref, green_ref)):
            for plane in range(2):
                for half in range(halves):
                    for column in range(inner):
                        begin = column * local_rows
                        packed_ref[field, plane, half, begin : begin + local_rows, :] = ref[
                            plane, side * halves + half, column
                        ]


def stage_kernel(
    blocks_ref, onsite_ref, energies_ref, table_in_ref, twiddle_in_ref,
    causal_ref, energy_ref, onsite_out_ref, table_ref, twiddle_ref
):
    ta, ka = lax.axis_index("ta"), lax.axis_index("ka")
    table_ref[...] = table_in_ref[...]
    twiddle_ref[...] = twiddle_in_ref[...]
    local_rows, all_times, k_local = causal_ref.shape[0], causal_ref.shape[1], energy_ref.shape[1]
    for side, begin in enumerate((ka * k_local, (1 - ka) * k_local)):
        energy_ref[side : side + 1, :] = energies_ref[
            :, pl.ds(pl.multiple_of(begin, LANES), k_local)
        ]
    orbitals = onsite_ref.shape[1]
    halves = orbitals // 2
    for row in range(orbitals):
        for column in range(orbitals):
            for plane in range(2):
                value = onsite_ref[
                    plane, (row + ka * halves) % orbitals, (column + ka * halves) % orbitals
                ]
                place = (plane * orbitals + row) * orbitals + column
                onsite_out_ref[place : place + 1, :] = jnp.full((1, LANES), value)
    for stored in range(local_rows):
        row_time = blocks_ref[ta] * local_rows + stored
        for column in range(all_times):
            column_time = blocks_ref[column // local_rows] * local_rows + column % local_rows
            seen = jnp.where(row_time <= column_time, jnp.float32(1.0), jnp.float32(0.0))
            causal_ref[stored, column : column + 1, :] = jnp.full((1, LANES), seen)


def opening_kernel(
    own_ref, other_ref, table_ref, twiddle_ref, screens_ref, sigma_ref, send_ref
):
    halves, k_local = own_ref.shape[2], own_ref.shape[4]
    local_tiles = k_local // LANES
    spaces = []
    for field in range(3):
        rows = []
        for half in range(halves):
            near = tiles_of(lambda p, ds: own_ref[field, p, half, :, ds], local_tiles)
            far = tiles_of(lambda p, ds: other_ref[field, p, half, :, ds], local_tiles)
            rows.append(near + far)
        spaces.append(to_sites(rows, table_ref, twiddle_ref))
    screens_ref[0] = spaces[0]
    screens_ref[1] = spaces[1]
    emit_sigma(
        lax.axis_index("ka"), spaces[2], screens_ref, table_ref, twiddle_ref, sigma_ref, send_ref
    )


def rate_pieces(own_side, half, tile, onsite_ref, energy, near_ref, far_ref, sums_refs):
    halves = near_ref.shape[1]
    orbitals = 2 * halves
    lanes = pl.ds(tile * LANES, LANES)
    row = half if own_side else halves + half
    here = near_ref if own_side else far_ref
    real_part = functools.reduce(jnp.add, [ref[0, half, :, lanes] for ref in sums_refs])
    imag_part = functools.reduce(jnp.add, [ref[1, half, :, lanes] for ref in sums_refs])
    real_part = real_part + energy * here[0, half, :, lanes]
    imag_part = imag_part + energy * here[1, half, :, lanes]
    for side, ref in enumerate((near_ref, far_ref)):
        for column in range(halves):
            place = row * orbitals + side * halves + column
            coupling_real = onsite_ref[place : place + 1, :]
            place += orbitals * orbitals
            coupling_imag = onsite_ref[place : place + 1, :]
            value_real, value_imag = ref[0, column, :, lanes], ref[1, column, :, lanes]
            real_part = real_part + coupling_real * value_real - coupling_imag * value_imag
            imag_part = imag_part + coupling_real * value_imag + coupling_imag * value_real
    return imag_part, -real_part


def advance_kernel(
    is_first, near_count, far_count, onsite_ref, energy_ref, near_here_ref, far_here_ref,
    near_there_ref, far_there_ref, green_here_ref, green_there_ref, screens_ref, table_ref,
    twiddle_ref, *refs
):
    sums_here, refs = refs[:near_count], refs[near_count:]
    sums_there, refs = refs[:far_count], refs[far_count:]
    first_here_ref, first_there_ref, estimate_ref, sigma_ref, send_ref = refs
    halves, k_local = near_here_ref.shape[1], near_here_ref.shape[3]
    local_tiles = k_local // LANES
    fields = []
    places = (
        (0, near_here_ref, far_here_ref, green_here_ref, first_here_ref, sums_here),
        (1, near_there_ref, far_there_ref, green_there_ref, first_there_ref, sums_there),
    )
    for half in range(halves):
        parts = []
        for side, near_ref, far_ref, green_ref, first_ref, sums_refs in places:
            for tile in range(local_tiles):
                lanes = pl.ds(tile * LANES, LANES)
                energy = energy_ref[side : side + 1, lanes]
                rates = rate_pieces(
                    True, half, tile, onsite_ref, energy, near_ref, far_ref, sums_refs
                )
                pair = []
                for plane in range(2):
                    start = green_ref[plane, half, :, lanes]
                    if is_first:
                        first_ref[plane, half, :, lanes] = rates[plane]
                        value = start + time_step * rates[plane]
                    else:
                        value = start + 0.5 * time_step * (
                            first_ref[plane, half, :, lanes] + rates[plane]
                        )
                    estimate_ref[side, plane, half, :, lanes] = value
                    if side == 1 and not is_first:
                        estimate_ref[2, plane, half, :, lanes] = first_ref[plane, half, :, lanes]
                    pair.append(value)
                parts.append(tuple(pair))
        fields.append(parts)
    space = to_sites(fields, table_ref, twiddle_ref)
    emit_sigma(
        lax.axis_index("ka"), space, screens_ref, table_ref, twiddle_ref, sigma_ref, send_ref
    )


def closing_kernel(
    near_count, far_count, onsite_ref, energy_ref, near_ref, far_ref, green_near_ref,
    green_far_ref, first_near_ref, first_far_ref, *refs
):
    ka = lax.axis_index("ka")
    near_sums, far_sums = refs[:near_count], refs[near_count : near_count + far_count]
    next_ref, latest_ref = refs[near_count + far_count :]
    halves, k_local = near_ref.shape[1], near_ref.shape[3]
    sides = (
        (True, ka, near_sums, green_near_ref, first_near_ref),
        (False, 1 - ka, far_sums, green_far_ref, first_far_ref),
    )
    for own_side, side, sums_refs, green_ref, first_ref in sides:
        for half in range(halves):
            for tile in range(k_local // LANES):
                lanes = pl.ds(tile * LANES, LANES)
                energy = energy_ref[0:1, lanes]
                rates = rate_pieces(
                    own_side, half, tile, onsite_ref, energy, near_ref, far_ref, sums_refs
                )
                for plane in range(2):
                    value = green_ref[plane, half, :, lanes] + 0.5 * time_step * (
                        first_ref[plane, half, :, lanes] + rates[plane]
                    )
                    for column in range(next_ref.shape[2]):
                        begin = column * next_ref.shape[3]
                        span = slice(begin, begin + next_ref.shape[3])
                        latest_ref[plane, side * halves + half, column, :, lanes] = rates[plane][span]
                        next_ref[plane, side * halves + half, column, :, lanes] = value[span]


def swap_rows(values, local_rows):
    count = len(values)
    group = lax.broadcasted_iota(jnp.int32, (SUBLANES, LANES), 0) // local_rows
    values = list(values)
    step = 1
    while step < count:
        low = (group & step) == 0
        for place in range(count):
            if place & step == 0:
                first, second = values[place], values[place | step]
                shift = step * local_rows
                values[place] = jnp.where(low, first, pltpu.roll(second, shift, 0))
                values[place | step] = jnp.where(
                    low, pltpu.roll(first, SUBLANES - shift, 0), second
                )
        step *= 2
    return values


def collide_kernel(
    order, sigma_ref, causal_ref, lesser_ref, advanced_ref, keep_ref, send_ref
):
    halves, k_local = sigma_ref.shape[2], sigma_ref.shape[4]
    orbitals, local_rows, times = lesser_ref.shape[1], lesser_ref.shape[3], lesser_ref.shape[4]
    rows = SUBLANES
    time_steps = times // rows
    me = lax.axis_index("ta")

    def gather(total, value):
        return value if total is None else total + value

    def step(counter, carried):
        tile = counter % time_steps
        here = pl.ds(pl.multiple_of(tile * rows, rows), rows)
        lanes = pl.ds(pl.multiple_of(counter // time_steps * LANES, LANES), LANES)
        sums = [[[None] * 3 for _ in range(orbitals)] for _ in range(halves)]
        for field, slab_ref in ((1, lesser_ref), (0, advanced_ref)):
            for stored in range(local_rows):
                for inner in range(orbitals):
                    row = inner * local_rows + stored
                    sigmas = []
                    for half in range(halves):
                        triple = [
                            jnp.broadcast_to(
                                sigma_ref[field, plane, half, row : row + 1, lanes], (rows, LANES)
                            )
                            for plane in range(2)
                        ]
                        if field == 0:
                            triple = [value * causal_ref[stored, here] for value in triple]
                        sigmas.append(triple + [triple[0] + triple[1]])
                    for outer in range(orbitals):
                        slabs = [
                            slab_ref[plane, inner, outer, stored, here, lanes].astype(jnp.float32)
                            for plane in range(2)
                        ]
                        slabs.append(slabs[0] + slabs[1])
                        for half in range(halves):
                            totals = sums[half][outer]
                            for term in range(3):
                                totals[term] = gather(
                                    totals[term], sigmas[half][term] * slabs[term]
                                )
        even = (me & 1) == 0
        for half in range(halves):
            real_parts = [totals[0] - totals[1] for totals in sums[half]]
            imag_parts = [totals[2] - (totals[0] + totals[1]) for totals in sums[half]]
            for plane, parts in ((0, real_parts), (1, imag_parts)):
                owners = swap_rows(parts, local_rows)
                for pair in range(0, orbitals, 2):
                    relative = (tile * orbitals + pair) ^ me
                    where_to = 0
                    for bit in order[1:]:
                        where_to = where_to * 2 + ((relative >> bit) & 1)
                    first, second = owners[pair], owners[pair + 1]
                    keep_ref[where_to, plane, half, :, lanes] = jnp.where(even, first, second)
                    send_ref[where_to, plane, half, :, lanes] = jnp.where(even, second, first)
        return carried

    lax.fori_loop(0, time_steps * (k_local // LANES), step, 0)


def whole(memory_space=pltpu.VMEM):
    return pl.BlockSpec(memory_space=memory_space)


def float_like(*shape):
    return jax.ShapeDtypeStruct(shape, jnp.float32)


def flip(bit, count):
    return [(place, place ^ bit) for place in range(count)]


def halved_sum(keep, send, order, direct_bits, ta_count, ka_count=None):
    got = lax.ppermute(send, "ta", flip(1 << order[0], ta_count))
    for bit in order[1 : len(order) - direct_bits]:
        half = keep.shape[0] // 2
        outgoing, keep = keep[half:] + got[half:], keep[:half] + got[:half]
        got = lax.ppermute(outgoing, "ta", flip(1 << bit, ta_count))
    if direct_bits == 0:
        return keep[0], got[0]
    shift = order[-1]
    pieces = [keep[place] + got[place] for place in range(1 << direct_bits)]
    results = []
    for place in range(1 << direct_bits):
        across = place << shift
        if ka_count is not None:
            pairs = flip(across * ka_count + 1, ta_count * ka_count)
            results.append(lax.ppermute(pieces[place], ("ta", "ka"), pairs))
        elif place == 0:
            results.append(pieces[0])
        else:
            results.append(lax.ppermute(pieces[place], "ta", flip(across, ta_count)))
    return tuple(results)


def fast(
    green_row, screen_lesser, screen_retarded, onsite, lesser_slab, advanced_slab, slab_start,
    block_table
):
    orbitals, local_rows, k_local = green_row.shape[1], green_row.shape[3], green_row.shape[4]
    ta_count, ka_count = lax.axis_size("ta"), lax.axis_size("ka")
    all_times = local_rows * ta_count
    halves = orbitals // 2
    tiles = k_local * ka_count // LANES
    table, twiddle = fourier_tables(tiles)
    momenta = jnp.arange(KS * KS, dtype=jnp.int32)
    start = lax.optimization_barrier(jnp.broadcast_to(slab_start, momenta.shape))
    energies = dispersion(start[None], all_times, momenta // KS, momenta % KS)[None]

    chunk = (2, halves, SUBLANES, k_local)
    scalar = whole(pltpu.SMEM)
    space_rows = halves * tiles * SUBLANES
    sigma_shape = float_like(2, *chunk)
    small = pltpu.CompilerParams(vmem_limit_bytes=8 * 1024 * 1024)

    hint = pl.CostEstimate(
        flops=8 * lesser_slab.size, bytes_accessed=8 * lesser_slab.size, transcendentals=0
    )
    near_fields, far_fields = pl.pallas_call(
        pack_kernel,
        out_shape=(float_like(3, *chunk),) * 2,
        in_specs=[whole()] * 3,
        out_specs=(whole(),) * 2,
        compiler_params=small,
        cost_estimate=hint,
        name="pack",
    )(screen_lesser, screen_retarded, green_row)
    arrived_fields = lax.ppermute(far_fields, "ka", flip(1, ka_count))
    causal, energy, onsite, table, twiddle = pl.pallas_call(
        stage_kernel,
        out_shape=(
            float_like(local_rows, all_times, LANES),
            float_like(2, k_local),
            float_like(2 * orbitals * orbitals, LANES),
            jax.ShapeDtypeStruct(table.shape, table.dtype),
            jax.ShapeDtypeStruct(twiddle.shape, twiddle.dtype),
        ),
        in_specs=[scalar] * 2 + [whole()] * 3,
        out_specs=(whole(),) * 5,
        compiler_params=small,
        cost_estimate=hint,
        name="stage",
    )(block_table, onsite, energies, table, twiddle)
    green_near, green_far, green_there = near_fields[2], far_fields[2], arrived_fields[2]

    screens, sigma_near, sigma_send = pl.pallas_call(
        opening_kernel,
        out_shape=(float_like(2, space_rows, 2 * LANES), sigma_shape, sigma_shape),
        in_specs=[whole()] * 4,
        out_specs=(whole(),) * 3,
        compiler_params=small,
        cost_estimate=hint,
        name="opening",
    )(near_fields, arrived_fields, table, twiddle)

    bits = ta_count.bit_length() - 1
    owner_bits = orbitals.bit_length() - 1
    order = list(range(owner_bits)) + list(range(owner_bits, bits))[::-1]
    direct_bits = bits - owner_bits

    def collide(sigma):
        return pl.pallas_call(
            functools.partial(collide_kernel, order),
            out_shape=(float_like(ta_count // 2, *chunk),) * 2,
            in_specs=[whole()] * 4,
            out_specs=(whole(),) * 2,
            compiler_params=small,
            cost_estimate=pl.CostEstimate(
                flops=16 * halves * orbitals * orbitals * local_rows * all_times * k_local,
                bytes_accessed=4 * lesser_slab.size,
                transcendentals=0,
            ),
            name="collide",
        )(sigma, causal, lesser_slab, advanced_slab)

    def exchanged(value):
        return lax.ppermute(value, "ka", flip(1, ka_count))

    def collisions(sigma_near, sigma_send, crossing):
        sigma_far = exchanged(sigma_send)
        near = collide(sigma_near)
        far = collide(sigma_far)
        near_sums = halved_sum(*near, order, 0, ta_count)
        far_sums = halved_sum(*far, order, direct_bits, ta_count, crossing)
        return near_sums, far_sums

    chunk_shape = float_like(*chunk)
    near_here, near_there, far_here = green_near, green_there, green_far
    far_there = None
    first_here = first_there = None
    for corrector in range(2):
        is_first = corrector == 0
        near_sums, far_sums = collisions(sigma_near, sigma_send, ka_count)
        if is_first:
            far_there = exchanged(green_near)
        else:
            swapped = exchanged(estimate)
            far_here, far_there = swapped[1], swapped[0]
        outputs = (float_like(2 if is_first else 3, *chunk), sigma_shape, sigma_shape)
        inputs = (
            onsite, energy, near_here, far_here, near_there, far_there, green_near,
            green_there, screens, table, twiddle, *near_sums, *far_sums,
        )
        if is_first:
            outputs = (chunk_shape,) * 2 + outputs
        else:
            inputs = inputs + (first_here, first_there)
        result = pl.pallas_call(
            functools.partial(advance_kernel, is_first, len(near_sums), len(far_sums)),
            out_shape=outputs,
            in_specs=[whole()] * len(inputs),
            out_specs=(whole(),) * len(outputs),
            compiler_params=small,
            name="advance",
        )(*inputs)
        if is_first:
            first_here, first_there = result[:2]
        estimate, sigma_near, sigma_send = result[-3:]
        near_here, near_there = estimate[0], estimate[1]
    near_sums, far_sums = collisions(sigma_near, sigma_send, None)
    swapped = exchanged(estimate[1:])
    far_here, first_far = swapped[0], swapped[1]
    full = float_like(*green_row.shape)
    return pl.pallas_call(
        functools.partial(closing_kernel, len(near_sums), len(far_sums)),
        out_shape=(full, full),
        in_specs=[whole()] * (8 + len(near_sums) + len(far_sums)),
        out_specs=(whole(), whole()),
        compiler_params=small,
        name="closing",
    )(
        onsite, energy, near_here, far_here, green_near, green_far, first_here, first_far,
        *near_sums, *far_sums,
    )


def local(*args):
    if suits(args[0], lax.axis_size("ta"), lax.axis_size("ka")):
        return fast(*args)
    return plain(*args)


def solution(mesh):
    return jax.shard_map(
        local,
        mesh=mesh,
        in_specs=(
            P(None, None, None, "ta", "ka"),
            P(None, None, None, "ta", "ka"),
            P(None, None, None, "ta", "ka"),
            P(),
            P(None, None, None, "ta", None, "ka"),
            P(None, None, None, "ta", None, "ka"),
            P(),
            P(),
        ),
        out_specs=(P(None, None, None, "ta", "ka"), P(None, None, None, "ta", "ka")),
        check_vma=False,
    )
```

```python
import functools
import math

import jax
import jax.numpy as jnp
import numpy as np
from jax import lax
from jax.experimental import pallas as pl
from jax.experimental.pallas import tpu as pltpu
from jax.sharding import PartitionSpec as P

KS = 32
LANES = 128
SUBLANES = 8


time_step = 0.1
drive_amp = 1.0
drive_freq = 0.37
highest = lax.Precision.HIGHEST


def phase_table(row_ids, col_ids, sign_value):
    products = row_ids[:, None] * col_ids[None, :] % KS
    angle = products.astype(jnp.float32) * (2.0 * math.pi / KS)
    factor = 1.0 / math.sqrt(KS)
    return (jnp.cos(angle) * factor, sign_value * jnp.sin(angle) * factor)


def along_last(values_in, cosine, sine_part):
    real_part = jnp.einsum("...m,mn->...n", values_in[0], cosine, precision=highest) - jnp.einsum(
        "...m,mn->...n", values_in[1], sine_part, precision=highest
    )
    imag_part = jnp.einsum(
        "...m,mn->...n", values_in[0], sine_part, precision=highest
    ) + jnp.einsum("...m,mn->...n", values_in[1], cosine, precision=highest)
    return jnp.stack([real_part, imag_part])


def along_second(values_in, cosine, sine_part):
    real_part = jnp.einsum("...mj,mn->...nj", values_in[0], cosine, precision=highest) - jnp.einsum(
        "...mj,mn->...nj", values_in[1], sine_part, precision=highest
    )
    imag_part = jnp.einsum(
        "...mj,mn->...nj", values_in[0], sine_part, precision=highest
    ) + jnp.einsum("...mj,mn->...nj", values_in[1], cosine, precision=highest)
    return jnp.stack([real_part, imag_part])


def transform(values_in, sign_value, ka_index):
    leading = values_in.shape[:-1]
    x_local = values_in.shape[-1] // KS
    numbers = jnp.arange(KS, dtype=jnp.int32)
    owned = ka_index * x_local + jnp.arange(x_local, dtype=jnp.int32)
    cosine, sine_part = phase_table(numbers, numbers, sign_value)
    partly = along_last(values_in.reshape(leading + (x_local, KS)), cosine, sine_part)
    gathered = lax.all_gather(partly.reshape(values_in.shape), "ka", axis=5, tiled=True)
    grid = gathered.reshape(leading + (KS, KS))
    col_cos, col_sin = phase_table(numbers, owned, sign_value)
    return along_second(grid, col_cos, col_sin).reshape(values_in.shape)


def self_energy(row_space, screens):
    green_real = row_space[0][None]
    green_imag = row_space[1][None]
    real_part = -(green_real * screens[1] + green_imag * screens[0])
    imag_part = green_real * screens[0] - green_imag * screens[1]
    return jnp.stack([real_part, imag_part])


def coupling(sigma_pair):
    return jnp.stack(
        [jnp.stack([sigma_pair[0], -sigma_pair[1]]), jnp.stack([sigma_pair[1], sigma_pair[0]])]
    )


def dispersion(slab_start, all_times, kx_ids, ky_ids):
    current = (slab_start[0] + all_times).astype(jnp.float32)
    shift = drive_amp * jnp.sin(drive_freq * current)
    factor = 2.0 * math.pi / KS
    return -2.0 * (
        jnp.cos(kx_ids.astype(jnp.float32) * factor + shift)
        + jnp.cos(ky_ids.astype(jnp.float32) * factor)
    )


def apply_h(row, onsite, energy):
    real_part = (
        jnp.einsum("ab,bctk->actk", onsite[0], row[0], precision=highest)
        - jnp.einsum("ab,bctk->actk", onsite[1], row[1], precision=highest)
        + energy * row[0]
    )
    imag_part = (
        jnp.einsum("ab,bctk->actk", onsite[0], row[1], precision=highest)
        + jnp.einsum("ab,bctk->actk", onsite[1], row[0], precision=highest)
        + energy * row[1]
    )
    return jnp.stack([real_part, imag_part])


def masked_product(less_coupling, row_times, piece_times, piece_adv):
    visible = row_times[:, None] <= piece_times[None, :]
    masked = jnp.where(visible[:, :, None], piece_adv, jnp.zeros_like(piece_adv))
    return jnp.einsum(
        "pqabsk,qbcstk->tpack", less_coupling, masked, preferred_element_type=jnp.float32
    )


def plain(
    green_row,
    screen_lesser,
    screen_retarded,
    onsite,
    lesser_slab,
    advanced_slab,
    slab_start,
    block_table,
):
    local_rows = green_row.shape[3]
    k_local = green_row.shape[4]
    ta_count = lax.axis_size("ta")
    all_times = local_rows * ta_count
    my_index = lax.axis_index("ta")
    ka_index = lax.axis_index("ka")
    my_block = lax.dynamic_slice_in_dim(block_table, my_index, 1)[0]
    row_times = my_block * local_rows + jnp.arange(local_rows, dtype=jnp.int32)
    col_times = jnp.repeat(block_table, local_rows) * local_rows + jnp.tile(
        jnp.arange(local_rows, dtype=jnp.int32), ta_count
    )
    momenta = ka_index * k_local + jnp.arange(k_local, dtype=jnp.int32)
    energy = dispersion(slab_start, all_times, momenta // KS, momenta % KS)
    first_space = transform(
        jnp.stack([screen_lesser, screen_retarded, green_row], axis=1), 1.0, ka_index
    )
    screens = first_space[:, 0:2]

    def rate_of(row, row_space):
        sigma_all = transform(self_energy(row_space, screens), -1.0, ka_index).astype(jnp.bfloat16)
        less_coupling = coupling(sigma_all[:, 0])
        ret_coupling = coupling(sigma_all[:, 1])
        totals = jnp.einsum(
            "pqabsk,qbcstk->tpack", ret_coupling, lesser_slab, preferred_element_type=jnp.float32
        )
        own_rows = lax.psum_scatter(
            totals + masked_product(less_coupling, row_times, col_times, advanced_slab),
            "ta",
            scatter_dimension=0,
            tiled=True,
        )
        collision = jnp.transpose(own_rows, (1, 2, 3, 0, 4))
        totals = apply_h(row, onsite, energy) + collision
        return jnp.stack([totals[1], -totals[0]])

    first_rate = rate_of(green_row, first_space[:, 2])
    estimate = green_row + time_step * first_rate
    latest = first_rate
    for _ in range(2):
        row_space = transform(estimate[:, None], 1.0, ka_index)[:, 0]
        latest = rate_of(estimate, row_space)
        estimate = green_row + 0.5 * time_step * (first_rate + latest)
    return (estimate, latest)


def halving(size):
    return size > 0 and size & (size - 1) == 0


def suits(green_row, ta_count, ka_count):
    orbitals, local_rows, k_local = green_row.shape[1], green_row.shape[3], green_row.shape[4]
    return (
        ka_count == 2
        and orbitals * local_rows == SUBLANES
        and orbitals >= 4
        and halving(orbitals)
        and halving(ta_count)
        and ta_count % (2 * orbitals) == 0
        and k_local % LANES == 0
        and halving(k_local // LANES)
        and LANES % KS == 0
        and k_local * ka_count == KS * KS
    )


def fourier_tables(tiles):
    lane = np.arange(LANES)
    outer, inner = lane // KS, lane % KS
    group = LANES // KS
    angle = 2.0 * np.pi * (
        (outer[:, None] * outer[None, :] % group) / group + (inner[:, None] * inner[None, :] % KS) / KS
    )
    cosine, sine = np.cos(angle) / KS, np.sin(angle) / KS
    full = np.block([[cosine, sine], [-sine, cosine]]).astype(np.float32)
    turn = 2.0 * np.pi * (outer[None, :] * np.arange(tiles)[:, None]) / KS
    twiddle = np.concatenate([np.cos(turn), np.sin(turn)], axis=1).astype(np.float32)
    full = np.concatenate([full, twiddle])
    high = full.astype(jnp.bfloat16)
    low = (full - high.astype(np.float32)).astype(jnp.bfloat16)
    return jnp.asarray(np.stack([high, low]))


def radix(values):
    count = len(values)
    if count == 1:
        return values
    half = count // 2
    sums, differences = [], []
    for place in range(half):
        (ar, ai), (br, bi) = values[place], values[place + half]
        sums.append((ar + br, ai + bi))
        dr, di = ar - br, ai - bi
        if place == 0:
            differences.append((dr, di))
        elif 4 * place == count:
            differences.append((-di, dr))
        else:
            cosine = math.cos(2.0 * math.pi * place / count)
            sine = math.sin(2.0 * math.pi * place / count)
            differences.append((dr * cosine - di * sine, dr * sine + di * cosine))
    even, odd = radix(sums), radix(differences)
    return [pair for both in zip(even, odd) for pair in both]


def turned(pair, twiddle_ref, tile):
    if tile == 0:
        return pair
    cosine, sine = twiddle_ref[tile : tile + 1, :LANES], twiddle_ref[tile : tile + 1, LANES:]
    return (pair[0] * cosine - pair[1] * sine, pair[0] * sine + pair[1] * cosine)


def lane_transform(rows, table_ref):
    high = rows.astype(jnp.bfloat16)
    low = (rows - high.astype(jnp.float32)).astype(jnp.bfloat16)
    first, second = table_ref[0], table_ref[1]
    dot = functools.partial(jnp.dot, preferred_element_type=jnp.float32)
    return dot(high, first) + (dot(low, first) + dot(high, second))


def to_sites(fields, table_ref, twiddle_ref):
    pieces = []
    for tiles in fields:
        for tile, pair in enumerate(radix(tiles)):
            pieces.append(jnp.concatenate(turned(pair, twiddle_ref, tile), axis=1))
    return lane_transform(jnp.concatenate(pieces, axis=0), table_ref)


def tiles_of(load, count):
    return [
        (load(0, pl.ds(tile * LANES, LANES)), load(1, pl.ds(tile * LANES, LANES)))
        for tile in range(count)
    ]


def emit_sigma(ka, space, screens_ref, table_ref, twiddle_ref, own_ref, send_ref):
    halves, k_local = own_ref.shape[2], own_ref.shape[4]
    local_tiles = k_local // LANES
    tiles = 2 * local_tiles
    green_real, green_imag = space[:, :LANES], space[:, LANES:]
    products = []
    for field in range(2):
        screen_real, screen_imag = screens_ref[field, :, :LANES], screens_ref[field, :, LANES:]
        real_part = -(green_real * screen_imag + green_imag * screen_real)
        conjugate = green_imag * screen_imag - green_real * screen_real
        products.append(jnp.concatenate([real_part, conjugate], axis=1))
    back = lane_transform(jnp.concatenate(products, axis=0), table_ref)
    for field in range(2):
        for half in range(halves):
            parts = []
            for tile in range(tiles):
                row = ((field * halves + half) * tiles + tile) * SUBLANES
                pair = (back[row : row + SUBLANES, :LANES], back[row : row + SUBLANES, LANES:])
                parts.append(turned(pair, twiddle_ref, tile))
            parts = radix(parts)
            for tile in range(local_tiles):
                for plane, sign in ((0, 1.0), (1, -1.0)):
                    near = (sign * parts[tile][plane]).astype(jnp.bfloat16).astype(jnp.float32)
                    far = (
                        (sign * parts[tile + local_tiles][plane])
                        .astype(jnp.bfloat16)
                        .astype(jnp.float32)
                    )
                    where_to = pl.ds(tile * LANES, LANES)
                    own_ref[field, plane, half, :, where_to] = jnp.where(ka == 0, near, far)
                    send_ref[field, plane, half, :, where_to] = jnp.where(ka == 0, far, near)


def pack_kernel(lesser_ref, retarded_ref, green_ref, near_ref, far_ref):
    ka = lax.axis_index("ka")
    halves, inner, local_rows = near_ref.shape[2], lesser_ref.shape[2], lesser_ref.shape[3]
    for side, packed_ref in ((1 - ka, far_ref), (ka, near_ref)):
        for field, ref in enumerate((lesser_ref, retarded_ref, green_ref)):
            for plane in range(2):
                for half in range(halves):
                    for column in range(inner):
                        begin = column * local_rows
                        packed_ref[field, plane, half, begin : begin + local_rows, :] = ref[
                            plane, side * halves + half, column
                        ]


def stage_kernel(
    blocks_ref, onsite_ref, lesser_ref, advanced_ref, energies_ref, tables_ref, held_ref, masked_ref,
    energy_ref, onsite_out_ref, table_ref, twiddle_ref
):
    ta, ka = lax.axis_index("ta"), lax.axis_index("ka")
    table_rows = table_ref.shape[1]
    table_ref[...] = tables_ref[:, :table_rows]
    turns = tables_ref[:, table_rows:].astype(jnp.float32)
    twiddle_ref[...] = turns[0] + turns[1]
    k_local = energy_ref.shape[1]
    planes, orbitals, _, local_rows, all_times, _ = lesser_ref.shape
    for side, begin in enumerate((ka * k_local, (1 - ka) * k_local)):
        energy_ref[side : side + 1, :] = energies_ref[
            :, pl.ds(pl.multiple_of(begin, LANES), k_local)
        ]
    halves = orbitals // 2
    for row in range(orbitals):
        for column in range(orbitals):
            for plane in range(2):
                value = onsite_ref[
                    plane, (row + ka * halves) % orbitals, (column + ka * halves) % orbitals
                ]
                place = (plane * orbitals + row) * orbitals + column
                onsite_out_ref[place : place + 1, :] = jnp.full((1, LANES), value)
    position = lax.broadcasted_iota(jnp.int32, (all_times, LANES), 0)
    column_times = jnp.zeros((all_times, LANES), jnp.int32)
    for block in range(all_times // local_rows):
        column_times = jnp.where(
            position // local_rows == block, blocks_ref[block] * local_rows, column_times
        )
    column_times = column_times + position % local_rows
    seen = [
        (blocks_ref[ta] * local_rows + stored <= column_times)
        .astype(jnp.float32)
        .astype(advanced_ref.dtype)
        for stored in range(local_rows)
    ]

    def move(counter, carried):
        plane = counter // (orbitals * orbitals)
        inner = counter // orbitals % orbitals
        outer = counter % orbitals
        for stored in range(local_rows):
            for tile in range(k_local // LANES):
                lanes = pl.ds(tile * LANES, LANES)
                held_ref[plane, inner, outer, stored, :, lanes] = lesser_ref[
                    plane, inner, outer, stored, :, lanes
                ]
                masked_ref[plane, inner, outer, stored, :, lanes] = (
                    advanced_ref[plane, inner, outer, stored, :, lanes] * seen[stored]
                )
        return carried

    lax.fori_loop(0, planes * orbitals * orbitals, move, 0)


def opening_kernel(
    own_ref, other_ref, table_ref, twiddle_ref, screens_ref, sigma_ref, send_ref
):
    halves, k_local = own_ref.shape[2], own_ref.shape[4]
    local_tiles = k_local // LANES
    spaces = []
    for field in range(3):
        rows = []
        for half in range(halves):
            near = tiles_of(lambda p, ds: own_ref[field, p, half, :, ds], local_tiles)
            far = tiles_of(lambda p, ds: other_ref[field, p, half, :, ds], local_tiles)
            rows.append(near + far)
        spaces.append(to_sites(rows, table_ref, twiddle_ref))
    screens_ref[0] = spaces[0]
    screens_ref[1] = spaces[1]
    emit_sigma(
        lax.axis_index("ka"), spaces[2], screens_ref, table_ref, twiddle_ref, sigma_ref, send_ref
    )


def rate_pieces(own_side, half, tile, onsite_ref, energy, near_ref, far_ref, sums_refs):
    halves = near_ref.shape[1]
    orbitals = 2 * halves
    lanes = pl.ds(tile * LANES, LANES)
    row = half if own_side else halves + half
    here = near_ref if own_side else far_ref
    real_part = functools.reduce(jnp.add, [ref[0, half, :, lanes] for ref in sums_refs])
    imag_part = functools.reduce(jnp.add, [ref[1, half, :, lanes] for ref in sums_refs])
    real_part = real_part + energy * here[0, half, :, lanes]
    imag_part = imag_part + energy * here[1, half, :, lanes]
    for side, ref in enumerate((near_ref, far_ref)):
        for column in range(halves):
            place = row * orbitals + side * halves + column
            coupling_real = onsite_ref[place : place + 1, :]
            place += orbitals * orbitals
            coupling_imag = onsite_ref[place : place + 1, :]
            value_real, value_imag = ref[0, column, :, lanes], ref[1, column, :, lanes]
            real_part = real_part + coupling_real * value_real - coupling_imag * value_imag
            imag_part = imag_part + coupling_real * value_imag + coupling_imag * value_real
    return imag_part, -real_part


def advance_kernel(
    is_first, near_count, far_count, onsite_ref, energy_ref, near_here_ref, far_here_ref,
    near_there_ref, far_there_ref, green_here_ref, green_there_ref, screens_ref, table_ref,
    twiddle_ref, *refs
):
    sums_here, refs = refs[:near_count], refs[near_count:]
    sums_there, refs = refs[:far_count], refs[far_count:]
    first_here_ref, first_there_ref, estimate_ref, sigma_ref, send_ref = refs
    halves, k_local = near_here_ref.shape[1], near_here_ref.shape[3]
    local_tiles = k_local // LANES
    fields = []
    places = (
        (0, near_here_ref, far_here_ref, green_here_ref, first_here_ref, sums_here),
        (1, near_there_ref, far_there_ref, green_there_ref, first_there_ref, sums_there),
    )
    for half in range(halves):
        parts = []
        for side, near_ref, far_ref, green_ref, first_ref, sums_refs in places:
            for tile in range(local_tiles):
                lanes = pl.ds(tile * LANES, LANES)
                energy = energy_ref[side : side + 1, lanes]
                rates = rate_pieces(
                    True, half, tile, onsite_ref, energy, near_ref, far_ref, sums_refs
                )
                pair = []
                for plane in range(2):
                    start = green_ref[plane, half, :, lanes]
                    if is_first:
                        first_ref[plane, half, :, lanes] = rates[plane]
                        value = start + time_step * rates[plane]
                    else:
                        value = start + 0.5 * time_step * (
                            first_ref[plane, half, :, lanes] + rates[plane]
                        )
                    estimate_ref[side, plane, half, :, lanes] = value
                    if side == 1 and not is_first:
                        estimate_ref[2, plane, half, :, lanes] = first_ref[plane, half, :, lanes]
                    pair.append(value)
                parts.append(tuple(pair))
        fields.append(parts)
    space = to_sites(fields, table_ref, twiddle_ref)
    emit_sigma(
        lax.axis_index("ka"), space, screens_ref, table_ref, twiddle_ref, sigma_ref, send_ref
    )


def closing_kernel(
    near_count, far_count, onsite_ref, energy_ref, near_ref, far_ref, green_near_ref,
    green_far_ref, first_near_ref, first_far_ref, *refs
):
    ka = lax.axis_index("ka")
    near_sums, far_sums = refs[:near_count], refs[near_count : near_count + far_count]
    next_ref, latest_ref = refs[near_count + far_count :]
    halves, k_local = near_ref.shape[1], near_ref.shape[3]
    sides = (
        (True, ka, near_sums, green_near_ref, first_near_ref),
        (False, 1 - ka, far_sums, green_far_ref, first_far_ref),
    )
    for own_side, side, sums_refs, green_ref, first_ref in sides:
        for half in range(halves):
            for tile in range(k_local // LANES):
                lanes = pl.ds(tile * LANES, LANES)
                energy = energy_ref[0:1, lanes]
                rates = rate_pieces(
                    own_side, half, tile, onsite_ref, energy, near_ref, far_ref, sums_refs
                )
                for plane in range(2):
                    value = green_ref[plane, half, :, lanes] + 0.5 * time_step * (
                        first_ref[plane, half, :, lanes] + rates[plane]
                    )
                    for column in range(next_ref.shape[2]):
                        begin = column * next_ref.shape[3]
                        span = slice(begin, begin + next_ref.shape[3])
                        latest_ref[plane, side * halves + half, column, :, lanes] = rates[plane][span]
                        next_ref[plane, side * halves + half, column, :, lanes] = value[span]


def swap_rows(values, local_rows):
    count = len(values)
    group = lax.broadcasted_iota(jnp.int32, (SUBLANES, LANES), 0) // local_rows
    values = list(values)
    step = 1
    while step < count:
        low = (group & step) == 0
        for place in range(count):
            if place & step == 0:
                first, second = values[place], values[place | step]
                shift = step * local_rows
                values[place] = jnp.where(low, first, pltpu.roll(second, shift, 0))
                values[place | step] = jnp.where(
                    low, pltpu.roll(first, SUBLANES - shift, 0), second
                )
        step *= 2
    return values


def collide_kernel(
    order, sigma_ref, lesser_ref, advanced_ref, keep_ref, send_ref
):
    halves, k_local = sigma_ref.shape[2], sigma_ref.shape[4]
    orbitals, local_rows, times = lesser_ref.shape[1], lesser_ref.shape[3], lesser_ref.shape[4]
    rows = SUBLANES
    time_steps = times // rows
    me = lax.axis_index("ta")

    def gather(total, value):
        return value if total is None else total + value

    def step(counter, carried):
        tile = counter % time_steps
        here = pl.ds(pl.multiple_of(tile * rows, rows), rows)
        lanes = pl.ds(pl.multiple_of(counter // time_steps * LANES, LANES), LANES)
        sums = [[[None] * 3 for _ in range(orbitals)] for _ in range(halves)]
        for field, slab_ref in ((1, lesser_ref), (0, advanced_ref)):
            for stored in range(local_rows):
                for inner in range(orbitals):
                    row = inner * local_rows + stored
                    sigmas = []
                    for half in range(halves):
                        triple = [
                            jnp.broadcast_to(
                                sigma_ref[field, plane, half, row : row + 1, lanes], (rows, LANES)
                            )
                            for plane in range(2)
                        ]
                        sigmas.append(triple + [triple[0] + triple[1]])
                    for outer in range(orbitals):
                        slabs = [
                            slab_ref[plane, inner, outer, stored, here, lanes].astype(jnp.float32)
                            for plane in range(2)
                        ]
                        slabs.append(slabs[0] + slabs[1])
                        for half in range(halves):
                            totals = sums[half][outer]
                            for term in range(3):
                                totals[term] = gather(
                                    totals[term], sigmas[half][term] * slabs[term]
                                )
        even = (me & 1) == 0
        for half in range(halves):
            real_parts = [totals[0] - totals[1] for totals in sums[half]]
            imag_parts = [totals[2] - (totals[0] + totals[1]) for totals in sums[half]]
            for plane, parts in ((0, real_parts), (1, imag_parts)):
                owners = swap_rows(parts, local_rows)
                for pair in range(0, orbitals, 2):
                    relative = (tile * orbitals + pair) ^ me
                    where_to = 0
                    for bit in order[1:]:
                        where_to = where_to * 2 + ((relative >> bit) & 1)
                    first, second = owners[pair], owners[pair + 1]
                    keep_ref[where_to, plane, half, :, lanes] = jnp.where(even, first, second)
                    send_ref[where_to, plane, half, :, lanes] = jnp.where(even, second, first)
        return carried

    lax.fori_loop(0, time_steps * (k_local // LANES), step, 0)


def whole(memory_space=pltpu.VMEM):
    return pl.BlockSpec(memory_space=memory_space)


def float_like(*shape):
    return jax.ShapeDtypeStruct(shape, jnp.float32)


def flip(bit, count):
    return [(place, place ^ bit) for place in range(count)]


def halved_sum(keep, send, order, direct_bits, ta_count, ka_count=None):
    got = lax.ppermute(send, "ta", flip(1 << order[0], ta_count))
    for bit in order[1 : len(order) - direct_bits]:
        half = keep.shape[0] // 2
        outgoing, keep = keep[half:] + got[half:], keep[:half] + got[:half]
        got = lax.ppermute(outgoing, "ta", flip(1 << bit, ta_count))
    if direct_bits == 0:
        return keep[0], got[0]
    shift = order[-1]
    pieces = [keep[place] + got[place] for place in range(1 << direct_bits)]
    results = []
    for place in range(1 << direct_bits):
        across = place << shift
        if ka_count is not None:
            pairs = flip(across * ka_count + 1, ta_count * ka_count)
            results.append(lax.ppermute(pieces[place], ("ta", "ka"), pairs))
        elif place == 0:
            results.append(pieces[0])
        else:
            results.append(lax.ppermute(pieces[place], "ta", flip(across, ta_count)))
    return tuple(results)


def fast(
    green_row, screen_lesser, screen_retarded, onsite, lesser_slab, advanced_slab, slab_start,
    block_table
):
    orbitals, local_rows, k_local = green_row.shape[1], green_row.shape[3], green_row.shape[4]
    ta_count, ka_count = lax.axis_size("ta"), lax.axis_size("ka")
    all_times = local_rows * ta_count
    halves = orbitals // 2
    tiles = k_local * ka_count // LANES
    tables_in = fourier_tables(tiles)
    momenta = jnp.arange(KS * KS, dtype=jnp.int32)
    start = lax.optimization_barrier(jnp.broadcast_to(slab_start, momenta.shape))
    energies = dispersion(start[None], all_times, momenta // KS, momenta % KS)[None]

    chunk = (2, halves, SUBLANES, k_local)
    scalar = whole(pltpu.SMEM)
    space_rows = halves * tiles * SUBLANES
    sigma_shape = float_like(2, *chunk)
    small = pltpu.CompilerParams(vmem_limit_bytes=8 * 1024 * 1024)

    hint = pl.CostEstimate(
        flops=8 * lesser_slab.size, bytes_accessed=8 * lesser_slab.size, transcendentals=0
    )
    near_fields, far_fields = pl.pallas_call(
        pack_kernel,
        out_shape=(float_like(3, *chunk),) * 2,
        in_specs=[whole()] * 3,
        out_specs=(whole(),) * 2,
        compiler_params=small,
        cost_estimate=hint,
        name="pack",
    )(screen_lesser, screen_retarded, green_row)
    arrived_fields = lax.ppermute(far_fields, "ka", flip(1, ka_count))
    lesser_slab, advanced_slab, energy, onsite, table, twiddle = pl.pallas_call(
        stage_kernel,
        out_shape=(
            jax.ShapeDtypeStruct(lesser_slab.shape, lesser_slab.dtype),
            jax.ShapeDtypeStruct(advanced_slab.shape, advanced_slab.dtype),
            float_like(2, k_local),
            float_like(2 * orbitals * orbitals, LANES),
            jax.ShapeDtypeStruct((2, 2 * LANES, 2 * LANES), tables_in.dtype),
            float_like(tiles, 2 * LANES),
        ),
        in_specs=[scalar] * 2 + [whole()] * 4,
        out_specs=(whole(),) * 6,
        compiler_params=small,
        cost_estimate=hint,
        name="stage",
    )(block_table, onsite, lesser_slab, advanced_slab, energies, tables_in)
    green_near, green_far, green_there = near_fields[2], far_fields[2], arrived_fields[2]

    screens, sigma_near, sigma_send = pl.pallas_call(
        opening_kernel,
        out_shape=(float_like(2, space_rows, 2 * LANES), sigma_shape, sigma_shape),
        in_specs=[whole()] * 4,
        out_specs=(whole(),) * 3,
        compiler_params=small,
        cost_estimate=hint,
        name="opening",
    )(near_fields, arrived_fields, table, twiddle)

    bits = ta_count.bit_length() - 1
    owner_bits = orbitals.bit_length() - 1
    order = list(range(owner_bits)) + list(range(owner_bits, bits))[::-1]
    direct_bits = bits - owner_bits

    def collide(sigma):
        return pl.pallas_call(
            functools.partial(collide_kernel, order),
            out_shape=(float_like(ta_count // 2, *chunk),) * 2,
            in_specs=[whole()] * 3,
            out_specs=(whole(),) * 2,
            compiler_params=small,
            cost_estimate=pl.CostEstimate(
                flops=16 * halves * orbitals * orbitals * local_rows * all_times * k_local,
                bytes_accessed=4 * lesser_slab.size,
                transcendentals=0,
            ),
            name="collide",
        )(sigma, lesser_slab, advanced_slab)

    def exchanged(value):
        return lax.ppermute(value, "ka", flip(1, ka_count))

    def collisions(sigma_near, sigma_send, crossing):
        sigma_far = exchanged(sigma_send)
        near = collide(sigma_near)
        far = collide(sigma_far)
        near_sums = halved_sum(*near, order, 0, ta_count)
        far_sums = halved_sum(*far, order, direct_bits, ta_count, crossing)
        return near_sums, far_sums

    chunk_shape = float_like(*chunk)
    near_here, near_there, far_here = green_near, green_there, green_far
    far_there = None
    first_here = first_there = None
    for corrector in range(2):
        is_first = corrector == 0
        near_sums, far_sums = collisions(sigma_near, sigma_send, ka_count)
        if is_first:
            far_there = exchanged(green_near)
        else:
            swapped = exchanged(estimate)
            far_here, far_there = swapped[1], swapped[0]
        outputs = (float_like(2 if is_first else 3, *chunk), sigma_shape, sigma_shape)
        inputs = (
            onsite, energy, near_here, far_here, near_there, far_there, green_near,
            green_there, screens, table, twiddle, *near_sums, *far_sums,
        )
        if is_first:
            outputs = (chunk_shape,) * 2 + outputs
        else:
            inputs = inputs + (first_here, first_there)
        result = pl.pallas_call(
            functools.partial(advance_kernel, is_first, len(near_sums), len(far_sums)),
            out_shape=outputs,
            in_specs=[whole()] * len(inputs),
            out_specs=(whole(),) * len(outputs),
            compiler_params=small,
            name="advance",
        )(*inputs)
        if is_first:
            first_here, first_there = result[:2]
        estimate, sigma_near, sigma_send = result[-3:]
        near_here, near_there = estimate[0], estimate[1]
    near_sums, far_sums = collisions(sigma_near, sigma_send, None)
    swapped = exchanged(estimate[1:])
    far_here, first_far = swapped[0], swapped[1]
    full = float_like(*green_row.shape)
    return pl.pallas_call(
        functools.partial(closing_kernel, len(near_sums), len(far_sums)),
        out_shape=(full, full),
        in_specs=[whole()] * (8 + len(near_sums) + len(far_sums)),
        out_specs=(whole(), whole()),
        compiler_params=small,
        name="closing",
    )(
        onsite, energy, near_here, far_here, green_near, green_far, first_here, first_far,
        *near_sums, *far_sums,
    )


def local(*args):
    if suits(args[0], lax.axis_size("ta"), lax.axis_size("ka")):
        return fast(*args)
    return plain(*args)


def solution(mesh):
    return jax.shard_map(
        local,
        mesh=mesh,
        in_specs=(
            P(None, None, None, "ta", "ka"),
            P(None, None, None, "ta", "ka"),
            P(None, None, None, "ta", "ka"),
            P(),
            P(None, None, None, "ta", None, "ka"),
            P(None, None, None, "ta", None, "ka"),
            P(),
            P(),
        ),
        out_specs=(P(None, None, None, "ta", "ka"), P(None, None, None, "ta", "ka")),
        check_vma=False,
    )
```

```python
import functools
import math

import jax
import jax.numpy as jnp
import numpy as np
from jax import lax
from jax.experimental import pallas as pl
from jax.experimental.pallas import tpu as pltpu
from jax.sharding import PartitionSpec as P

KS = 32
LANES = 128
SUBLANES = 8


time_step = 0.1
drive_amp = 1.0
drive_freq = 0.37
highest = lax.Precision.HIGHEST


def phase_table(row_ids, col_ids, sign_value):
    products = row_ids[:, None] * col_ids[None, :] % KS
    angle = products.astype(jnp.float32) * (2.0 * math.pi / KS)
    factor = 1.0 / math.sqrt(KS)
    return (jnp.cos(angle) * factor, sign_value * jnp.sin(angle) * factor)


def along_last(values_in, cosine, sine_part):
    real_part = jnp.einsum("...m,mn->...n", values_in[0], cosine, precision=highest) - jnp.einsum(
        "...m,mn->...n", values_in[1], sine_part, precision=highest
    )
    imag_part = jnp.einsum(
        "...m,mn->...n", values_in[0], sine_part, precision=highest
    ) + jnp.einsum("...m,mn->...n", values_in[1], cosine, precision=highest)
    return jnp.stack([real_part, imag_part])


def along_second(values_in, cosine, sine_part):
    real_part = jnp.einsum("...mj,mn->...nj", values_in[0], cosine, precision=highest) - jnp.einsum(
        "...mj,mn->...nj", values_in[1], sine_part, precision=highest
    )
    imag_part = jnp.einsum(
        "...mj,mn->...nj", values_in[0], sine_part, precision=highest
    ) + jnp.einsum("...mj,mn->...nj", values_in[1], cosine, precision=highest)
    return jnp.stack([real_part, imag_part])


def transform(values_in, sign_value, ka_index):
    leading = values_in.shape[:-1]
    x_local = values_in.shape[-1] // KS
    numbers = jnp.arange(KS, dtype=jnp.int32)
    owned = ka_index * x_local + jnp.arange(x_local, dtype=jnp.int32)
    cosine, sine_part = phase_table(numbers, numbers, sign_value)
    partly = along_last(values_in.reshape(leading + (x_local, KS)), cosine, sine_part)
    gathered = lax.all_gather(partly.reshape(values_in.shape), "ka", axis=5, tiled=True)
    grid = gathered.reshape(leading + (KS, KS))
    col_cos, col_sin = phase_table(numbers, owned, sign_value)
    return along_second(grid, col_cos, col_sin).reshape(values_in.shape)


def self_energy(row_space, screens):
    green_real = row_space[0][None]
    green_imag = row_space[1][None]
    real_part = -(green_real * screens[1] + green_imag * screens[0])
    imag_part = green_real * screens[0] - green_imag * screens[1]
    return jnp.stack([real_part, imag_part])


def coupling(sigma_pair):
    return jnp.stack(
        [jnp.stack([sigma_pair[0], -sigma_pair[1]]), jnp.stack([sigma_pair[1], sigma_pair[0]])]
    )


def dispersion(slab_start, all_times, kx_ids, ky_ids):
    current = (slab_start[0] + all_times).astype(jnp.float32)
    shift = drive_amp * jnp.sin(drive_freq * current)
    factor = 2.0 * math.pi / KS
    return -2.0 * (
        jnp.cos(kx_ids.astype(jnp.float32) * factor + shift)
        + jnp.cos(ky_ids.astype(jnp.float32) * factor)
    )


def apply_h(row, onsite, energy):
    real_part = (
        jnp.einsum("ab,bctk->actk", onsite[0], row[0], precision=highest)
        - jnp.einsum("ab,bctk->actk", onsite[1], row[1], precision=highest)
        + energy * row[0]
    )
    imag_part = (
        jnp.einsum("ab,bctk->actk", onsite[0], row[1], precision=highest)
        + jnp.einsum("ab,bctk->actk", onsite[1], row[0], precision=highest)
        + energy * row[1]
    )
    return jnp.stack([real_part, imag_part])


def masked_product(less_coupling, row_times, piece_times, piece_adv):
    visible = row_times[:, None] <= piece_times[None, :]
    masked = jnp.where(visible[:, :, None], piece_adv, jnp.zeros_like(piece_adv))
    return jnp.einsum(
        "pqabsk,qbcstk->tpack", less_coupling, masked, preferred_element_type=jnp.float32
    )


def plain(
    green_row,
    screen_lesser,
    screen_retarded,
    onsite,
    lesser_slab,
    advanced_slab,
    slab_start,
    block_table,
):
    local_rows = green_row.shape[3]
    k_local = green_row.shape[4]
    ta_count = lax.axis_size("ta")
    all_times = local_rows * ta_count
    my_index = lax.axis_index("ta")
    ka_index = lax.axis_index("ka")
    my_block = lax.dynamic_slice_in_dim(block_table, my_index, 1)[0]
    row_times = my_block * local_rows + jnp.arange(local_rows, dtype=jnp.int32)
    col_times = jnp.repeat(block_table, local_rows) * local_rows + jnp.tile(
        jnp.arange(local_rows, dtype=jnp.int32), ta_count
    )
    momenta = ka_index * k_local + jnp.arange(k_local, dtype=jnp.int32)
    energy = dispersion(slab_start, all_times, momenta // KS, momenta % KS)
    first_space = transform(
        jnp.stack([screen_lesser, screen_retarded, green_row], axis=1), 1.0, ka_index
    )
    screens = first_space[:, 0:2]

    def rate_of(row, row_space):
        sigma_all = transform(self_energy(row_space, screens), -1.0, ka_index).astype(jnp.bfloat16)
        less_coupling = coupling(sigma_all[:, 0])
        ret_coupling = coupling(sigma_all[:, 1])
        totals = jnp.einsum(
            "pqabsk,qbcstk->tpack", ret_coupling, lesser_slab, preferred_element_type=jnp.float32
        )
        own_rows = lax.psum_scatter(
            totals + masked_product(less_coupling, row_times, col_times, advanced_slab),
            "ta",
            scatter_dimension=0,
            tiled=True,
        )
        collision = jnp.transpose(own_rows, (1, 2, 3, 0, 4))
        totals = apply_h(row, onsite, energy) + collision
        return jnp.stack([totals[1], -totals[0]])

    first_rate = rate_of(green_row, first_space[:, 2])
    estimate = green_row + time_step * first_rate
    latest = first_rate
    for _ in range(2):
        row_space = transform(estimate[:, None], 1.0, ka_index)[:, 0]
        latest = rate_of(estimate, row_space)
        estimate = green_row + 0.5 * time_step * (first_rate + latest)
    return (estimate, latest)


def halving(size):
    return size > 0 and size & (size - 1) == 0


def suits(green_row, ta_count, ka_count):
    orbitals, local_rows, k_local = green_row.shape[1], green_row.shape[3], green_row.shape[4]
    return (
        ka_count == 2
        and orbitals * local_rows == SUBLANES
        and orbitals >= 4
        and halving(orbitals)
        and halving(ta_count)
        and ta_count % (2 * orbitals) == 0
        and k_local % LANES == 0
        and halving(k_local // LANES)
        and LANES % KS == 0
        and k_local * ka_count == KS * KS
    )


def fourier_tables(tiles):
    lane = np.arange(LANES)
    outer, inner = lane // KS, lane % KS
    group = LANES // KS
    angle = 2.0 * np.pi * (
        (outer[:, None] * outer[None, :] % group) / group + (inner[:, None] * inner[None, :] % KS) / KS
    )
    cosine, sine = np.cos(angle) / KS, np.sin(angle) / KS
    full = np.block([[cosine, sine], [-sine, cosine]]).astype(np.float32)
    turn = 2.0 * np.pi * (outer[None, :] * np.arange(tiles)[:, None]) / KS
    twiddle = np.concatenate([np.cos(turn), np.sin(turn)], axis=1).astype(np.float32)
    full = np.concatenate([full, twiddle])
    high = full.astype(jnp.bfloat16)
    low = (full - high.astype(np.float32)).astype(jnp.bfloat16)
    return jnp.asarray(np.stack([high, low]))


def radix(values):
    count = len(values)
    if count == 1:
        return values
    half = count // 2
    sums, differences = [], []
    for place in range(half):
        (ar, ai), (br, bi) = values[place], values[place + half]
        sums.append((ar + br, ai + bi))
        dr, di = ar - br, ai - bi
        if place == 0:
            differences.append((dr, di))
        elif 4 * place == count:
            differences.append((-di, dr))
        else:
            cosine = math.cos(2.0 * math.pi * place / count)
            sine = math.sin(2.0 * math.pi * place / count)
            differences.append((dr * cosine - di * sine, dr * sine + di * cosine))
    even, odd = radix(sums), radix(differences)
    return [pair for both in zip(even, odd) for pair in both]


def turned(pair, twiddle_ref, tile):
    if tile == 0:
        return pair
    cosine, sine = twiddle_ref[tile : tile + 1, :LANES], twiddle_ref[tile : tile + 1, LANES:]
    return (pair[0] * cosine - pair[1] * sine, pair[0] * sine + pair[1] * cosine)


def lane_transform(rows, table_ref):
    high = rows.astype(jnp.bfloat16)
    low = (rows - high.astype(jnp.float32)).astype(jnp.bfloat16)
    first, second = table_ref[0], table_ref[1]
    dot = functools.partial(jnp.dot, preferred_element_type=jnp.float32)
    return dot(high, first) + (dot(low, first) + dot(high, second))


def to_sites(fields, table_ref, twiddle_ref):
    pieces = []
    for tiles in fields:
        for tile, pair in enumerate(radix(tiles)):
            pieces.append(jnp.concatenate(turned(pair, twiddle_ref, tile), axis=1))
    return lane_transform(jnp.concatenate(pieces, axis=0), table_ref)


def tiles_of(load, count):
    return [
        (load(0, pl.ds(tile * LANES, LANES)), load(1, pl.ds(tile * LANES, LANES)))
        for tile in range(count)
    ]


def emit_sigma(ka, space, screens_ref, table_ref, twiddle_ref, own_ref, send_ref):
    halves, k_local = own_ref.shape[2], own_ref.shape[4]
    local_tiles = k_local // LANES
    tiles = 2 * local_tiles
    green_real, green_imag = space[:, :LANES], space[:, LANES:]
    products = []
    for field in range(2):
        screen_real, screen_imag = screens_ref[field, :, :LANES], screens_ref[field, :, LANES:]
        real_part = -(green_real * screen_imag + green_imag * screen_real)
        conjugate = green_imag * screen_imag - green_real * screen_real
        products.append(jnp.concatenate([real_part, conjugate], axis=1))
    back = lane_transform(jnp.concatenate(products, axis=0), table_ref)
    for field in range(2):
        for half in range(halves):
            parts = []
            for tile in range(tiles):
                row = ((field * halves + half) * tiles + tile) * SUBLANES
                pair = (back[row : row + SUBLANES, :LANES], back[row : row + SUBLANES, LANES:])
                parts.append(turned(pair, twiddle_ref, tile))
            parts = radix(parts)
            for tile in range(local_tiles):
                for plane, sign in ((0, 1.0), (1, -1.0)):
                    near = (sign * parts[tile][plane]).astype(jnp.bfloat16).astype(jnp.float32)
                    far = (
                        (sign * parts[tile + local_tiles][plane])
                        .astype(jnp.bfloat16)
                        .astype(jnp.float32)
                    )
                    where_to = pl.ds(tile * LANES, LANES)
                    own_ref[field, plane, half, :, where_to] = jnp.where(ka == 0, near, far)
                    send_ref[field, plane, half, :, where_to] = jnp.where(ka == 0, far, near)


def pack_kernel(lesser_ref, retarded_ref, green_ref, near_ref, far_ref):
    ka = lax.axis_index("ka")
    halves, inner, local_rows = near_ref.shape[2], lesser_ref.shape[2], lesser_ref.shape[3]
    for side, packed_ref in ((1 - ka, far_ref), (ka, near_ref)):
        for field, ref in enumerate((lesser_ref, retarded_ref, green_ref)):
            for plane in range(2):
                for half in range(halves):
                    for column in range(inner):
                        begin = column * local_rows
                        packed_ref[field, plane, half, begin : begin + local_rows, :] = ref[
                            plane, side * halves + half, column
                        ]


def couple_kernel(onsite_ref, energies_ref, energy_ref, onsite_out_ref):
    ka = lax.axis_index("ka")
    orbitals, k_local = onsite_ref.shape[1], energy_ref.shape[1]
    halves = orbitals // 2
    for side, begin in enumerate((ka * k_local, (1 - ka) * k_local)):
        energy_ref[side : side + 1, :] = energies_ref[
            :, pl.ds(pl.multiple_of(begin, LANES), k_local)
        ]
    for row in range(orbitals):
        for column in range(orbitals):
            for plane in range(2):
                value = onsite_ref[
                    plane, (row + ka * halves) % orbitals, (column + ka * halves) % orbitals
                ]
                place = (plane * orbitals + row) * orbitals + column
                onsite_out_ref[place : place + 1, :] = jnp.full((1, LANES), value)


def stage_kernel(
    blocks_ref, lesser_ref, advanced_ref, tables_ref, held_ref, masked_ref, table_ref, twiddle_ref
):
    ta = lax.axis_index("ta")
    table_rows = table_ref.shape[1]
    table_ref[...] = tables_ref[:, :table_rows]
    turns = tables_ref[:, table_rows:].astype(jnp.float32)
    twiddle_ref[...] = turns[0] + turns[1]
    planes, orbitals, _, local_rows, all_times, k_local = lesser_ref.shape
    position = lax.broadcasted_iota(jnp.int32, (all_times, LANES), 0)
    column_times = jnp.zeros((all_times, LANES), jnp.int32)
    for block in range(all_times // local_rows):
        column_times = jnp.where(
            position // local_rows == block, blocks_ref[block] * local_rows, column_times
        )
    column_times = column_times + position % local_rows
    seen = [
        (blocks_ref[ta] * local_rows + stored <= column_times)
        .astype(jnp.float32)
        .astype(advanced_ref.dtype)
        for stored in range(local_rows)
    ]

    def move(counter, carried):
        plane = counter // (orbitals * orbitals)
        inner = counter // orbitals % orbitals
        outer = counter % orbitals
        for stored in range(local_rows):
            for tile in range(k_local // LANES):
                lanes = pl.ds(tile * LANES, LANES)
                held_ref[plane, inner, outer, stored, :, lanes] = lesser_ref[
                    plane, inner, outer, stored, :, lanes
                ]
                masked_ref[plane, inner, outer, stored, :, lanes] = (
                    advanced_ref[plane, inner, outer, stored, :, lanes] * seen[stored]
                )
        return carried

    lax.fori_loop(0, planes * orbitals * orbitals, move, 0)


def opening_kernel(
    own_ref, other_ref, table_ref, twiddle_ref, screens_ref, sigma_ref, send_ref
):
    halves, k_local = own_ref.shape[2], own_ref.shape[4]
    local_tiles = k_local // LANES
    spaces = []
    for field in range(3):
        rows = []
        for half in range(halves):
            near = tiles_of(lambda p, ds: own_ref[field, p, half, :, ds], local_tiles)
            far = tiles_of(lambda p, ds: other_ref[field, p, half, :, ds], local_tiles)
            rows.append(near + far)
        spaces.append(to_sites(rows, table_ref, twiddle_ref))
    screens_ref[0] = spaces[0]
    screens_ref[1] = spaces[1]
    emit_sigma(
        lax.axis_index("ka"), spaces[2], screens_ref, table_ref, twiddle_ref, sigma_ref, send_ref
    )


def rate_pieces(own_side, half, tile, onsite_ref, energy, near_ref, far_ref, sums_refs):
    halves = near_ref.shape[1]
    orbitals = 2 * halves
    lanes = pl.ds(tile * LANES, LANES)
    row = half if own_side else halves + half
    here = near_ref if own_side else far_ref
    real_part = functools.reduce(jnp.add, [ref[0, half, :, lanes] for ref in sums_refs])
    imag_part = functools.reduce(jnp.add, [ref[1, half, :, lanes] for ref in sums_refs])
    real_part = real_part + energy * here[0, half, :, lanes]
    imag_part = imag_part + energy * here[1, half, :, lanes]
    for side, ref in enumerate((near_ref, far_ref)):
        for column in range(halves):
            place = row * orbitals + side * halves + column
            coupling_real = onsite_ref[place : place + 1, :]
            place += orbitals * orbitals
            coupling_imag = onsite_ref[place : place + 1, :]
            value_real, value_imag = ref[0, column, :, lanes], ref[1, column, :, lanes]
            real_part = real_part + coupling_real * value_real - coupling_imag * value_imag
            imag_part = imag_part + coupling_real * value_imag + coupling_imag * value_real
    return imag_part, -real_part


def advance_kernel(
    is_first, near_count, far_count, onsite_ref, energy_ref, near_here_ref, far_here_ref,
    near_there_ref, far_there_ref, green_here_ref, green_there_ref, screens_ref, table_ref,
    twiddle_ref, *refs
):
    sums_here, refs = refs[:near_count], refs[near_count:]
    sums_there, refs = refs[:far_count], refs[far_count:]
    first_here_ref, first_there_ref, estimate_ref, sigma_ref, send_ref = refs
    halves, k_local = near_here_ref.shape[1], near_here_ref.shape[3]
    local_tiles = k_local // LANES
    fields = []
    places = (
        (0, near_here_ref, far_here_ref, green_here_ref, first_here_ref, sums_here),
        (1, near_there_ref, far_there_ref, green_there_ref, first_there_ref, sums_there),
    )
    for half in range(halves):
        parts = []
        for side, near_ref, far_ref, green_ref, first_ref, sums_refs in places:
            for tile in range(local_tiles):
                lanes = pl.ds(tile * LANES, LANES)
                energy = energy_ref[side : side + 1, lanes]
                rates = rate_pieces(
                    True, half, tile, onsite_ref, energy, near_ref, far_ref, sums_refs
                )
                pair = []
                for plane in range(2):
                    start = green_ref[plane, half, :, lanes]
                    if is_first:
                        first_ref[plane, half, :, lanes] = rates[plane]
                        value = start + time_step * rates[plane]
                    else:
                        value = start + 0.5 * time_step * (
                            first_ref[plane, half, :, lanes] + rates[plane]
                        )
                    estimate_ref[side, plane, half, :, lanes] = value
                    if side == 1 and not is_first:
                        estimate_ref[2, plane, half, :, lanes] = first_ref[plane, half, :, lanes]
                    pair.append(value)
                parts.append(tuple(pair))
        fields.append(parts)
    space = to_sites(fields, table_ref, twiddle_ref)
    emit_sigma(
        lax.axis_index("ka"), space, screens_ref, table_ref, twiddle_ref, sigma_ref, send_ref
    )


def closing_kernel(
    near_count, far_count, onsite_ref, energy_ref, near_ref, far_ref, green_near_ref,
    green_far_ref, first_near_ref, first_far_ref, *refs
):
    ka = lax.axis_index("ka")
    near_sums, far_sums = refs[:near_count], refs[near_count : near_count + far_count]
    next_ref, latest_ref = refs[near_count + far_count :]
    halves, k_local = near_ref.shape[1], near_ref.shape[3]
    sides = (
        (True, ka, near_sums, green_near_ref, first_near_ref),
        (False, 1 - ka, far_sums, green_far_ref, first_far_ref),
    )
    for own_side, side, sums_refs, green_ref, first_ref in sides:
        for half in range(halves):
            for tile in range(k_local // LANES):
                lanes = pl.ds(tile * LANES, LANES)
                energy = energy_ref[0:1, lanes]
                rates = rate_pieces(
                    own_side, half, tile, onsite_ref, energy, near_ref, far_ref, sums_refs
                )
                for plane in range(2):
                    value = green_ref[plane, half, :, lanes] + 0.5 * time_step * (
                        first_ref[plane, half, :, lanes] + rates[plane]
                    )
                    for column in range(next_ref.shape[2]):
                        begin = column * next_ref.shape[3]
                        span = slice(begin, begin + next_ref.shape[3])
                        latest_ref[plane, side * halves + half, column, :, lanes] = rates[plane][span]
                        next_ref[plane, side * halves + half, column, :, lanes] = value[span]


def swap_rows(values, local_rows):
    count = len(values)
    group = lax.broadcasted_iota(jnp.int32, (SUBLANES, LANES), 0) // local_rows
    values = list(values)
    step = 1
    while step < count:
        low = (group & step) == 0
        for place in range(count):
            if place & step == 0:
                first, second = values[place], values[place | step]
                shift = step * local_rows
                values[place] = jnp.where(low, first, pltpu.roll(second, shift, 0))
                values[place | step] = jnp.where(
                    low, pltpu.roll(first, SUBLANES - shift, 0), second
                )
        step *= 2
    return values


def collide_kernel(
    order, sigma_ref, lesser_ref, advanced_ref, keep_ref, send_ref, summed_ref
):
    halves, k_local = sigma_ref.shape[2], sigma_ref.shape[4]
    orbitals, local_rows, times = lesser_ref.shape[1], lesser_ref.shape[3], lesser_ref.shape[4]
    rows = SUBLANES
    time_steps = times // rows
    me = lax.axis_index("ta")
    summed_ref[...] = sigma_ref[:, 0] + sigma_ref[:, 1]

    def gather(total, value):
        return value if total is None else total + value

    def step(counter, carried):
        tile = counter % time_steps
        here = pl.ds(pl.multiple_of(tile * rows, rows), rows)
        lanes = pl.ds(pl.multiple_of(counter // time_steps * LANES, LANES), LANES)
        sums = [[[None] * 3 for _ in range(orbitals)] for _ in range(halves)]
        for field, slab_ref in ((1, lesser_ref), (0, advanced_ref)):
            for stored in range(local_rows):
                for inner in range(orbitals):
                    row = inner * local_rows + stored
                    sigmas = []
                    for half in range(halves):
                        triple = [
                            jnp.broadcast_to(
                                sigma_ref[field, plane, half, row : row + 1, lanes], (rows, LANES)
                            )
                            for plane in range(2)
                        ]
                        both = summed_ref[field, half, row : row + 1, lanes]
                        sigmas.append(triple + [jnp.broadcast_to(both, (rows, LANES))])
                    for outer in range(orbitals):
                        slabs = [
                            slab_ref[plane, inner, outer, stored, here, lanes].astype(jnp.float32)
                            for plane in range(2)
                        ]
                        slabs.append(slabs[0] + slabs[1])
                        for half in range(halves):
                            totals = sums[half][outer]
                            for term in range(3):
                                totals[term] = gather(
                                    totals[term], sigmas[half][term] * slabs[term]
                                )
        even = (me & 1) == 0
        for half in range(halves):
            real_parts = [totals[0] - totals[1] for totals in sums[half]]
            imag_parts = [totals[2] - (totals[0] + totals[1]) for totals in sums[half]]
            for plane, parts in ((0, real_parts), (1, imag_parts)):
                owners = swap_rows(parts, local_rows)
                for pair in range(0, orbitals, 2):
                    relative = (tile * orbitals + pair) ^ me
                    where_to = 0
                    for bit in order[1:]:
                        where_to = where_to * 2 + ((relative >> bit) & 1)
                    first, second = owners[pair], owners[pair + 1]
                    keep_ref[where_to, plane, half, :, lanes] = jnp.where(even, first, second)
                    send_ref[where_to, plane, half, :, lanes] = jnp.where(even, second, first)
        return carried

    lax.fori_loop(0, time_steps * (k_local // LANES), step, 0)


def whole(memory_space=pltpu.VMEM):
    return pl.BlockSpec(memory_space=memory_space)


def float_like(*shape):
    return jax.ShapeDtypeStruct(shape, jnp.float32)


def flip(bit, count):
    return [(place, place ^ bit) for place in range(count)]


def halved_sum(keep, send, order, direct_bits, ta_count, ka_count=None):
    got = lax.ppermute(send, "ta", flip(1 << order[0], ta_count))
    for bit in order[1 : len(order) - direct_bits]:
        half = keep.shape[0] // 2
        outgoing, keep = keep[half:] + got[half:], keep[:half] + got[:half]
        got = lax.ppermute(outgoing, "ta", flip(1 << bit, ta_count))
    if direct_bits == 0:
        return keep[0], got[0]
    shift = order[-1]
    pieces = [keep[place] + got[place] for place in range(1 << direct_bits)]
    results = []
    for place in range(1 << direct_bits):
        across = place << shift
        if ka_count is not None:
            pairs = flip(across * ka_count + 1, ta_count * ka_count)
            results.append(lax.ppermute(pieces[place], ("ta", "ka"), pairs))
        elif place == 0:
            results.append(pieces[0])
        else:
            results.append(lax.ppermute(pieces[place], "ta", flip(across, ta_count)))
    return tuple(results)


def fast(
    green_row, screen_lesser, screen_retarded, onsite, lesser_slab, advanced_slab, slab_start,
    block_table
):
    orbitals, local_rows, k_local = green_row.shape[1], green_row.shape[3], green_row.shape[4]
    ta_count, ka_count = lax.axis_size("ta"), lax.axis_size("ka")
    all_times = local_rows * ta_count
    halves = orbitals // 2
    tiles = k_local * ka_count // LANES
    tables_in = fourier_tables(tiles)
    momenta = jnp.arange(KS * KS, dtype=jnp.int32)
    start = lax.optimization_barrier(jnp.broadcast_to(slab_start, momenta.shape))
    energies = dispersion(start[None], all_times, momenta // KS, momenta % KS)[None]

    chunk = (2, halves, SUBLANES, k_local)
    scalar = whole(pltpu.SMEM)
    space_rows = halves * tiles * SUBLANES
    sigma_shape = float_like(2, *chunk)
    small = pltpu.CompilerParams(vmem_limit_bytes=8 * 1024 * 1024)

    hint = pl.CostEstimate(
        flops=8 * lesser_slab.size, bytes_accessed=8 * lesser_slab.size, transcendentals=0
    )
    near_fields, far_fields = pl.pallas_call(
        pack_kernel,
        out_shape=(float_like(3, *chunk),) * 2,
        in_specs=[whole()] * 3,
        out_specs=(whole(),) * 2,
        compiler_params=small,
        cost_estimate=hint,
        name="pack",
    )(screen_lesser, screen_retarded, green_row)
    arrived_fields = lax.ppermute(far_fields, "ka", flip(1, ka_count))
    lesser_slab, advanced_slab, table, twiddle = pl.pallas_call(
        stage_kernel,
        out_shape=(
            jax.ShapeDtypeStruct(lesser_slab.shape, lesser_slab.dtype),
            jax.ShapeDtypeStruct(advanced_slab.shape, advanced_slab.dtype),
            jax.ShapeDtypeStruct((2, 2 * LANES, 2 * LANES), tables_in.dtype),
            float_like(tiles, 2 * LANES),
        ),
        in_specs=[scalar] + [whole()] * 3,
        out_specs=(whole(),) * 4,
        compiler_params=small,
        cost_estimate=hint,
        name="stage",
    )(block_table, lesser_slab, advanced_slab, tables_in)
    green_near, green_far, green_there = near_fields[2], far_fields[2], arrived_fields[2]

    screens, sigma_near, sigma_send = pl.pallas_call(
        opening_kernel,
        out_shape=(float_like(2, space_rows, 2 * LANES), sigma_shape, sigma_shape),
        in_specs=[whole()] * 4,
        out_specs=(whole(),) * 3,
        compiler_params=small,
        cost_estimate=hint,
        name="opening",
    )(near_fields, arrived_fields, table, twiddle)

    bits = ta_count.bit_length() - 1
    owner_bits = orbitals.bit_length() - 1
    order = list(range(owner_bits)) + list(range(owner_bits, bits))[::-1]
    direct_bits = bits - owner_bits

    def collide(sigma):
        return pl.pallas_call(
            functools.partial(collide_kernel, order),
            out_shape=(float_like(ta_count // 2, *chunk),) * 2,
            in_specs=[whole()] * 3,
            out_specs=(whole(),) * 2,
            scratch_shapes=[pltpu.VMEM((2,) + chunk[1:], jnp.float32)],
            compiler_params=small,
            cost_estimate=pl.CostEstimate(
                flops=16 * halves * orbitals * orbitals * local_rows * all_times * k_local,
                bytes_accessed=4 * lesser_slab.size,
                transcendentals=0,
            ),
            name="collide",
        )(sigma, lesser_slab, advanced_slab)

    def exchanged(value):
        return lax.ppermute(value, "ka", flip(1, ka_count))

    def collisions(sigma_near, sigma_send, crossing):
        sigma_far = exchanged(sigma_send)
        near = collide(sigma_near)
        far = collide(sigma_far)
        near_sums = halved_sum(*near, order, 0, ta_count)
        far_sums = halved_sum(*far, order, direct_bits, ta_count, crossing)
        return near_sums, far_sums

    chunk_shape = float_like(*chunk)
    near_here, near_there, far_here = green_near, green_there, green_far
    far_there = None
    first_here = first_there = None
    for corrector in range(2):
        is_first = corrector == 0
        near_sums, far_sums = collisions(sigma_near, sigma_send, ka_count)
        if is_first:
            energy, onsite = pl.pallas_call(
                couple_kernel,
                out_shape=(
                    float_like(2, k_local), float_like(2 * orbitals * orbitals, LANES)
                ),
                in_specs=[scalar, whole()],
                out_specs=(whole(),) * 2,
                compiler_params=small,
                name="couple",
            )(onsite, energies)
            far_there = exchanged(green_near)
        else:
            swapped = exchanged(estimate)
            far_here, far_there = swapped[1], swapped[0]
        outputs = (float_like(2 if is_first else 3, *chunk), sigma_shape, sigma_shape)
        inputs = (
            onsite, energy, near_here, far_here, near_there, far_there, green_near,
            green_there, screens, table, twiddle, *near_sums, *far_sums,
        )
        if is_first:
            outputs = (chunk_shape,) * 2 + outputs
        else:
            inputs = inputs + (first_here, first_there)
        result = pl.pallas_call(
            functools.partial(advance_kernel, is_first, len(near_sums), len(far_sums)),
            out_shape=outputs,
            in_specs=[whole()] * len(inputs),
            out_specs=(whole(),) * len(outputs),
            compiler_params=small,
            name="advance",
        )(*inputs)
        if is_first:
            first_here, first_there = result[:2]
        estimate, sigma_near, sigma_send = result[-3:]
        near_here, near_there = estimate[0], estimate[1]
    near_sums, far_sums = collisions(sigma_near, sigma_send, None)
    swapped = exchanged(estimate[1:])
    far_here, first_far = swapped[0], swapped[1]
    full = float_like(*green_row.shape)
    return pl.pallas_call(
        functools.partial(closing_kernel, len(near_sums), len(far_sums)),
        out_shape=(full, full),
        in_specs=[whole()] * (8 + len(near_sums) + len(far_sums)),
        out_specs=(whole(), whole()),
        compiler_params=small,
        name="closing",
    )(
        onsite, energy, near_here, far_here, green_near, green_far, first_here, first_far,
        *near_sums, *far_sums,
    )


def local(*args):
    if suits(args[0], lax.axis_size("ta"), lax.axis_size("ka")):
        return fast(*args)
    return plain(*args)


def solution(mesh):
    return jax.shard_map(
        local,
        mesh=mesh,
        in_specs=(
            P(None, None, None, "ta", "ka"),
            P(None, None, None, "ta", "ka"),
            P(None, None, None, "ta", "ka"),
            P(),
            P(None, None, None, "ta", None, "ka"),
            P(None, None, None, "ta", None, "ka"),
            P(),
            P(),
        ),
        out_specs=(P(None, None, None, "ta", "ka"), P(None, None, None, "ta", "ka")),
        check_vma=False,
    )
```
